8 devices in a mesh: dp: 2 (over y, z), sp: 4 (over x, core).
Axes of the slice: x: 2, y: 2, z: 1, core: 2. Of those that a mesh axis runs over, the one named last changes fastest.
Arguments:
- x: bfloat16 [8192, 4096], P(('dp', 'sp')), parts along dimension 0
- gain: bfloat16 [4096], replicated
- wq: bfloat16 [4096, 4096], P('sp')
- wk: bfloat16 [4096, 512], P('sp')
- wv: bfloat16 [4096, 512], P('sp')
- wo: bfloat16 [4096, 4096], P('sp')
Outputs:
- output: bfloat16 [8192, 4096], P(('dp', 'sp')), parts along dimension 0
There are 2 independent parts. The reference program is written for one: setup_inputs(seed, part) draws one part's arguments, and reference() takes and returns one part's arrays. A program takes and returns all parts, laid end to end along the dimension named above; an argument that names none is the same for every part.
All inputs are finite; a program needn't handle non-finite values.
Results may differ from the reference program's by a relative error of at most 0.012.
Values are sent between devices in bfloat16 or wider.
A program may use at most 2 GiB of HBM per device.

```python
import jax
import jax.numpy as jnp
from jax import lax

ROWS = 4096
D = 4096
HEADS = 32
KV_HEADS = 4
HEAD = 128
THETA = 10000


def setup_inputs(seed: int = 0, part: int = 0) -> dict:
    kx, kn, kq, kk, kv, ko = jax.random.split(jax.random.key(seed), 6)

    def weights(key, rows, columns):
        return jax.random.normal(key, (rows, columns), jnp.float32) * rows**-0.5

    drawn = {
        "x": jax.random.normal(jax.random.fold_in(kx, part), (ROWS, D), jnp.float32),
        "gain": 1 + 0.1 * jax.random.normal(kn, (D,), jnp.float32),
        "wq": 2 * weights(kq, D, HEADS * HEAD),
        "wk": 2 * weights(kk, D, KV_HEADS * HEAD),
        "wv": 4 * weights(kv, D, KV_HEADS * HEAD),
        "wo": weights(ko, HEADS * HEAD, D),
    }
    return {k: v.astype(jnp.bfloat16) for k, v in drawn.items()}


def normed(x, gain):
    wide = x.astype(jnp.float32)
    scale = lax.rsqrt(jnp.mean(wide * wide, -1, keepdims=True) + 1e-6)
    return (wide * scale * gain.astype(jnp.float32)).astype(jnp.bfloat16)


def turned(t, place, theta):
    half = t.shape[-1] // 2
    angle = place.astype(jnp.float32)[:, None] * theta ** (-jnp.arange(half, dtype=jnp.float32) / half)
    cos, sin = jnp.cos(angle)[:, None], jnp.sin(angle)[:, None]
    a, b = t[..., :half].astype(jnp.float32), t[..., half:].astype(jnp.float32)
    return jnp.concatenate([a * cos - b * sin, b * cos + a * sin], -1).astype(jnp.bfloat16)


def matmul(a, w):
    return jnp.dot(a, w, preferred_element_type=jnp.float32).astype(jnp.bfloat16)


def einsum(form, a, b):
    return jnp.einsum(form, a.astype(jnp.float32), b.astype(jnp.float32))


def attention(q, k, v):
    scores = einsum("tgsd,ugd->gstu", q, k) * q.shape[-1] ** -0.5
    token = jnp.arange(q.shape[0])
    scores = jnp.where(token[:, None] >= token, scores, -jnp.inf)
    weights = jax.nn.softmax(scores, -1).astype(jnp.bfloat16)
    return einsum("gstu,ugd->tgsd", weights, v).astype(jnp.bfloat16)


def reference(x, gain, wq, wk, wv, wo):
    a, place = normed(x, gain), jnp.arange(ROWS)
    q = turned(matmul(a, wq).reshape(ROWS, HEADS, HEAD), place, THETA).reshape(ROWS, KV_HEADS, -1, HEAD)
    k = turned(matmul(a, wk).reshape(ROWS, KV_HEADS, HEAD), place, THETA)
    v = matmul(a, wv).reshape(ROWS, KV_HEADS, HEAD)
    seen = attention(q, k, v).reshape(ROWS, HEADS * HEAD)
    return (x.astype(jnp.float32) + jnp.dot(seen, wo, preferred_element_type=jnp.float32)).astype(jnp.bfloat16)
```

```python
import functools

import jax
import jax.numpy as jnp
from jax import lax
from jax.experimental import pallas as pl
from jax.experimental.pallas import tpu as pltpu
from jax.sharding import PartitionSpec as P

HEAD = 128
THETA = 10000
LOG2E = 1.4426950408889634
HIDDEN = -2e30
OWN = 1024
D = 4096
CHIP = 2 * OWN
HALF = OWN // 2
COLS = 512
PIECES = 4
BLOCK = 512
BLOCKS = CHIP // BLOCK
HEADS = COLS // HEAD
MESH = pl.DeviceIdType.MESH
E = HEAD**-0.5 * LOG2E
WO = 4
WROWS = HALF // WO


def _dot(a, b, ca, cb):
    return lax.dot_general(a, b, (((ca,), (cb,)), ((), ())), preferred_element_type=jnp.float32)


def _kernel(x_ref, gain_ref, cos_ref, sin_ref, wq_ref, wk_ref, wv_ref, wo_ref, o_ref, wo_out,
            a_s, wq_s, wkv_s, k_s, v_s, q_s, mix_s, top_s, o_s,
            x_send, x_recv, y_send, y_recv, c_send, c_recv, own_sem, tok_sem, tok_send, tok_recv,
            kv_send, kv_recv, wx_send, wx_recv, wy_send, wy_recv, wc_send, wc_recv, wown_send, wown_recv, stage_in, stage_out,
            o_local, o_send, o_recv):
    y, d = lax.axis_index("dp"), lax.axis_index("sp")
    c, chip = lax.rem(d, 2), lax.div(d, 2)
    sib = d + 1 - 2 * c
    far = 2 * (1 - chip)
    par = far + c
    to_y, to_sib = {"dp": 1 - y}, {"sp": sib}

    def at(i, n, unit=None):
        return pl.ds(pl.multiple_of(i, unit or n), n)

    def remote(src, dst, send, recv, device):
        return pltpu.make_async_remote_copy(src_ref=src, dst_ref=dst, send_sem=send, recv_sem=recv, device_id=device, device_id_type=MESH)

    def arrived(ref, send, recv, device):
        remote(ref, ref, send, recv, device).wait_recv()

    def source(item, j, core, rows):
        if item == 0:
            return wk_ref.at[rows, at(core * 256, 256)]
        if item == 1:
            return wv_ref.at[rows, at(core * 256, 256)]
        return wq_ref.at[rows, at(core * 2048 + j * COLS, COLS)]

    def place(item, j, rows):
        return wkv_s.at[item, rows, :] if item in (0, 1) else wq_s.at[j, rows, :]

    def sem(item, j):
        return item if item in (0, 1) else 2 + j

    def x_copy(item, j, t):
        n = sem(item, j)
        return remote(source(item, j, t, at(y * HALF, HALF)), place(item, j, at(d * OWN + y * HALF, HALF)), x_send.at[n, t], x_recv.at[n, c],
                      {"sp": far + t})

    def send_x(item, j=0):
        for t in range(2):
            x_copy(item, j, t).start()

    def y_copy(item, j, s):
        n, here = sem(item, j), place(item, j, at((far + s) * OWN + y * HALF, HALF))
        return remote(here, here, y_send.at[n, s], y_recv.at[n, s], to_y)

    def hand_on(item, j=0):
        n = sem(item, j)
        for s in range(2):
            arrived(place(item, j, at((far + s) * OWN + y * HALF, HALF)), x_send.at[n, s], x_recv.at[n, s], {"sp": far + s})
            y_copy(item, j, s).start()

    def c_copy(item, j=0):
        n = sem(item, j)
        return remote(source(item, j, 1 - c, pl.ds(0, OWN)), place(item, j, at(d * OWN, OWN)), c_send.at[n], c_recv.at[n], to_sib)

    def own_copy(item, j=0):
        return pltpu.make_async_copy(source(item, j, c, pl.ds(0, OWN)), place(item, j, at(d * OWN, OWN)), own_sem.at[sem(item, j)])

    def complete(item, j=0):
        n = sem(item, j)
        own_copy(item, j).wait()
        arrived(place(item, j, at(sib * OWN, OWN)), c_send.at[n], c_recv.at[n], to_sib)
        for s in range(2):
            arrived(place(item, j, at((far + s) * OWN + (1 - y) * HALF, HALF)), y_send.at[n, s], y_recv.at[n, s], to_y)

    def sent(item, j=0):
        c_copy(item, j).wait_send()
        for s in range(2):
            x_copy(item, j, s).wait_send()
            y_copy(item, j, s).wait_send()

    def wo_x(s):
        return remote(wo_ref.at[at(y * HALF + s * WROWS, WROWS), :], wo_out.at[at(d * OWN + y * HALF + s * WROWS, WROWS), :], wx_send.at[s], wx_recv.at[s],
                      {"sp": par})

    def wo_rows(owner, half, s):
        return wo_out.at[at(owner * OWN + half * HALF + s * WROWS, WROWS), :]

    def wo_y(s):
        return remote(wo_rows(par, y, s), wo_rows(par, y, s), wy_send.at[s], wy_recv.at[s], to_y)

    def wo_c(s, by_y):
        here = wo_rows(par, 1 - y if by_y else y, s)
        return remote(here, here, wc_send.at[by_y, s], wc_recv.at[by_y, s], to_sib)

    def wo_hand_x(s):
        arrived(wo_rows(par, y, s), wx_send.at[s], wx_recv.at[s], {"sp": par})
        wo_y(s).start()
        wo_c(s, 0).start()

    def wo_hand_y(s):
        arrived(wo_rows(par, 1 - y, s), wy_send.at[s], wy_recv.at[s], to_y)
        wo_c(s, 1).start()

    wo_own = remote(wo_ref, wo_out.at[at(d * OWN, OWN), :], wown_send, wown_recv, to_sib)

    def stage(i, into):
        cols, slot = pl.ds((i % 8) * 512, 512), i % 4
        mid = o_s.at[slot // 2, pl.ds((slot % 2) * OWN, OWN), :]
        if into:
            return pltpu.make_async_copy(wo_ref.at[:, cols], mid, stage_in.at[slot])
        return pltpu.make_async_copy(mid, wo_out.at[at(d * OWN, OWN), cols], stage_out.at[slot])

    barrier = pltpu.get_barrier_semaphore()
    for device in (to_sib, {"sp": far}, {"sp": far + 1}, to_y):
        pl.semaphore_signal(barrier, inc=1, device_id=device, device_id_type=MESH)
    tokens = pltpu.make_async_copy(x_ref, a_s.at[at(c * OWN, OWN), :], tok_sem)
    tokens.start()
    pl.semaphore_wait(barrier, 4)
    send_x(0)
    send_x(1)
    send_x(2, 0)
    send_x(2, 1)
    c_copy(0).start()
    c_copy(1).start()
    x_copy_sib = remote(x_ref, a_s.at[at(c * OWN, OWN), :], tok_send, tok_recv, to_sib)
    x_copy_sib.start()
    own_copy(0).start()
    own_copy(1).start()
    for j in range(PIECES):
        c_copy(2, j).start()
        own_copy(2, j).start()
    wo_own.start()
    for i in range(4):
        stage(i, True).start()
    for g in range(2):
        v_s[g, HEAD:, :] = jnp.ones((16, 2 * CHIP), jnp.bfloat16)

    def norm(first):
        @pl.loop(0, OWN // 128)
        def _(i):
            rows = at(first + i * 128, 128)
            wide = a_s[rows, :].astype(jnp.float32)
            scale = lax.rsqrt(jnp.mean(wide * wide, -1, keepdims=True) + 1e-6)
            a_s[rows, :] = (wide * scale * gain_ref[...].astype(jnp.float32)).astype(jnp.bfloat16)

    tokens.wait()
    norm(c * OWN)
    for i in range(4):
        stage(i, True).wait()
        stage(i, False).start()
    hand_on(0)
    arrived(a_s.at[at(sib * OWN - 2 * chip * OWN, OWN), :], tok_send, tok_recv, to_sib)
    norm((1 - c) * OWN)
    hand_on(1)
    for i in range(4):
        stage(i, False).wait()
        stage(i + 4, True).start()

    def turn(t, m):
        rows = at(m * BLOCK, BLOCK)
        return (t * cos_ref[rows, :] + pltpu.roll(t, HEAD // 2, 1) * sin_ref[rows, :]).astype(jnp.bfloat16)

    complete(0)

    @pl.loop(0, BLOCKS)
    def _(m):
        t = _dot(a_s[at(m * BLOCK, BLOCK), :], wkv_s[0], 1, 0).astype(jnp.bfloat16).astype(jnp.float32)
        for g in range(2):
            k_s[g, at(chip * CHIP + m * BLOCK, BLOCK), :] = turn(t[:, g * HEAD : (g + 1) * HEAD], m)

    complete(1)

    @pl.loop(0, BLOCKS)
    def _(m):
        t = _dot(a_s[at(m * BLOCK, BLOCK), :], wkv_s[1], 1, 0)
        for g in range(2):
            v_s[g, :HEAD, at(chip * CHIP + m * BLOCK, BLOCK)] = t[:, g * HEAD : (g + 1) * HEAD].T.astype(jnp.bfloat16)

    def kv_copy(g, which):
        here = k_s.at[g, pl.ds(0, CHIP), :] if which == 0 else v_s.at[g, pl.ds(0, HEAD), pl.ds(0, CHIP)]
        return remote(here, here, kv_send.at[g, which], kv_recv.at[g, which], {"sp": c + 2})

    @pl.when(chip == 0)
    def _():
        for g in range(2):
            for which in range(2):
                kv_copy(g, which).start()

    send_x(2, 2)
    send_x(2, 3)
    for s in range(WO):
        wo_x(s).start()
    hand_on(2, 0)
    for i in range(4):
        stage(i + 4, True).wait()
        stage(i + 4, False).start()

    def block(g, qb, kb, first=False):
        keys = k_s[g, at(kb * BLOCK, BLOCK), :]
        values = v_s[g, :, at(kb * BLOCK, BLOCK)]
        scores = [_dot(keys, q_s[h, at(qb * BLOCK, BLOCK), :], 1, 1) for h in range(HEADS)]
        if first:
            seen = lax.broadcasted_iota(jnp.int32, (BLOCK, BLOCK), 0) <= lax.broadcasted_iota(jnp.int32, (BLOCK, BLOCK), 1)
        weights, keeps = [], []
        for h, s in enumerate(scores):
            if first:
                s = jnp.where(seen, s, HIDDEN)
                top = s.max(axis=0, keepdims=True)
            else:
                old = top_s[qb, h : h + 1, :]
                top = jnp.maximum(old, s.max(axis=0, keepdims=True))
                keeps.append(jnp.exp2((old - top) * E))
            top_s[qb, h : h + 1, :] = top
            weights.append(jnp.exp2((s - top) * E).astype(jnp.bfloat16))
        for h, p in enumerate(weights):
            new = _dot(values, p, 1, 0)
            mix_s[qb, h] = new if first else mix_s[qb, h] * keeps[h] + new

    def kv_arrived(g):
        for which in range(2):
            kv_copy(g, which).wait_recv()

    def o_out(j):
        slot = lax.rem(j, 2)
        cols = at(c * 2048 + j * COLS, COLS)
        local = pltpu.make_async_copy(o_s.at[slot, at(c * OWN, OWN), :], o_ref.at[:, cols], o_local.at[slot])
        away = remote(o_s.at[slot, at((1 - c) * OWN, OWN), :], o_ref.at[:, cols], o_send.at[slot], o_recv.at[j], to_sib)
        return local, away

    @pl.loop(0, PIECES)
    def _(j):
        g, slot = lax.div(j, 2), lax.rem(j, 2)
        complete(2, j)

        @pl.loop(0, BLOCKS)
        def _(m):
            t = _dot(a_s[at(m * BLOCK, BLOCK), :], wq_s[j], 1, 0).astype(jnp.bfloat16).astype(jnp.float32)
            for h in range(HEADS):
                q_s[h, at(m * BLOCK, BLOCK), :] = turn(t[:, h * HEAD : (h + 1) * HEAD], m)

        @pl.loop(0, BLOCKS)
        def _(qb):
            block(g, qb, chip * BLOCKS + qb, True)
            lax.fori_loop(0, qb, lambda i, _: block(g, qb, chip * BLOCKS + i), None)

        @pl.when(j < PIECES - 1)
        def _():
            hand_on(2, j + 1)

        @pl.when(j == 0)
        def _():
            for i in range(4):
                stage(i + 4, False).wait()

        @pl.when((chip == 1) & (j == 0))
        def _():
            kv_arrived(0)

        @pl.when((chip == 1) & (j == 2))
        def _():
            kv_arrived(1)

        @pl.when(j >= 2)
        def _():
            for copy, wait in zip(o_out(j - 2), ("wait", "wait_send")):
                getattr(copy, wait)()

        @pl.loop(0, BLOCKS)
        def _(qb):
            for s in range(WO):
                @pl.when((j == 2) & (qb == s))
                def _():
                    if s < 2:
                        pass
                    else:
                        wo_hand_x(s - 2)

                @pl.when((j == 3) & (qb == s))
                def _():
                    if s < 2:
                        wo_hand_y(s)
                        wo_hand_x(s + 2)

            lax.fori_loop(0, chip * BLOCKS, lambda i, _: block(g, qb, i), None)
            for h in range(HEADS):
                total = mix_s[qb, h, HEAD : HEAD + 1, :]
                o_s[slot, at(qb * BLOCK, BLOCK), h * HEAD : (h + 1) * HEAD] = (mix_s[qb, h, :HEAD, :] * (1 / total)).T.astype(jnp.bfloat16)

        for copy in o_out(j):
            copy.start()

    wo_hand_y(2)
    wo_hand_y(3)
    for j in range(PIECES):
        sent(2, j)
    sent(0)
    sent(1)

    @pl.when(chip == 0)
    def _():
        for g in range(2):
            for which in range(2):
                kv_copy(g, which).wait_send()

    x_copy_sib.wait_send()
    wo_own.wait_send()
    arrived(wo_out.at[at(sib * OWN, OWN), :], wown_send, wown_recv, to_sib)
    for s in range(WO):
        wo_x(s).wait_send()
        wo_y(s).wait_send()
        for by_y in range(2):
            wo_c(s, by_y).wait_send()
            arrived(wo_rows(far + 1 - c, 1 - y if by_y else y, s), wc_send.at[by_y, s], wc_recv.at[by_y, s], to_sib)
    for j in range(2, PIECES):
        local, away = o_out(j)
        local.wait()
        away.wait_send()
    for j in range(PIECES):
        arrived(o_ref.at[:, at((1 - c) * 2048 + j * COLS, COLS)], o_send.at[0], o_recv.at[j], to_sib)


def solution(mesh):
    dma = pltpu.SemaphoreType.DMA
    bf16, f32 = jnp.bfloat16, jnp.float32
    anywhere, vmem = pl.BlockSpec(memory_space=pl.ANY), pl.BlockSpec(memory_space=pltpu.VMEM)
    fused = pl.pallas_call(
        _kernel,
        in_specs=[anywhere, vmem, vmem, vmem, anywhere, anywhere, anywhere, anywhere],
        out_specs=[anywhere, anywhere],
        out_shape=[jax.ShapeDtypeStruct((OWN, D), bf16), jax.ShapeDtypeStruct((D, D), bf16)],
        scratch_shapes=[
            pltpu.VMEM((CHIP, D), bf16),
            pltpu.VMEM((PIECES, D, COLS), bf16),
            pltpu.VMEM((2, D, 256), bf16),
            pltpu.VMEM((2, 2 * CHIP, HEAD), bf16),
            pltpu.VMEM((2, HEAD + 16, 2 * CHIP), bf16),
            pltpu.VMEM((HEADS, CHIP, HEAD), bf16),
            pltpu.VMEM((BLOCKS, HEADS, HEAD + 16, BLOCK), f32),
            pltpu.VMEM((BLOCKS, HEADS, BLOCK), f32),
            pltpu.VMEM((2, CHIP, COLS), bf16),
            dma((6, 2)), dma((6, 2)), dma((6, 2)), dma((6, 2)), dma((6,)), dma((6,)), dma((6,)), dma, dma, dma,
            dma((2, 2)), dma((2, 2)), dma((WO,)), dma((WO,)), dma((WO,)), dma((WO,)), dma((2, WO)), dma((2, WO)), dma, dma, dma((4,)), dma((4,)),
            dma((2,)), dma((2,)), dma((PIECES,)),
        ],
        compiler_params=pltpu.CompilerParams(collective_id=0, has_side_effects=True, vmem_limit_bytes=67043328),
        cost_estimate=pl.CostEstimate(flops=140 * 10**9, transcendentals=10**8, bytes_accessed=10**8),
    )

    def step(x, gain, wq, wk, wv, wo):
        half = HEAD // 2
        place = lax.div(lax.axis_index("sp"), 2) * CHIP + jnp.arange(CHIP)
        angle = place.astype(f32)[:, None] * THETA ** (-jnp.arange(half, dtype=f32) / half)
        cos, sin = jnp.cos(angle), jnp.sin(angle)
        cos, sin = jnp.concatenate([cos, cos], -1), jnp.concatenate([-sin, sin], -1)
        seen, wo = fused(x, gain[None], cos, sin, wq, wk, wv, wo)
        return (x.astype(f32) + jnp.dot(seen, wo, preferred_element_type=f32)).astype(bf16)

    tokens, whole = P(("dp", "sp"), None), P("sp", None)
    return jax.shard_map(
        step,
        mesh=mesh,
        in_specs=(tokens, P(None), whole, whole, whole, whole),
        out_specs=tokens,
        check_vma=False,
    )
```

```python
import functools

import jax
import jax.numpy as jnp
from jax import lax
from jax.experimental import pallas as pl
from jax.experimental.pallas import tpu as pltpu
from jax.sharding import PartitionSpec as P

HEAD = 128
THETA = 10000
LOG2E = 1.4426950408889634
HIDDEN = -2e30
OWN = 1024
D = 4096
CHIP = 2 * OWN
HALF = OWN // 2
COLS = 512
PIECES = 4
BLOCK = 512
BLOCKS = CHIP // BLOCK
HEADS = COLS // HEAD
MESH = pl.DeviceIdType.MESH
E = HEAD**-0.5 * LOG2E
WO = D // COLS
PART = HALF // 2


def _dot(a, b, ca, cb):
    return lax.dot_general(a, b, (((ca,), (cb,)), ((), ())), preferred_element_type=jnp.float32)


def _kernel(x_ref, gain_ref, cos_ref, sin_ref, wq_ref, wk_ref, wv_ref, wo_ref, y_ref, wo_far,
            a_s, wq_s, pool_s, k_s, v_s, mix_s, top_s, o_s,
            x_send, x_recv, y_send, y_recv, c_send, c_recv, own_sem, tok_sem, tok_send, tok_recv,
            kv_send, kv_recv, wx_send, wx_recv, wy_send, wy_recv, wc_send, wc_recv, wown_send, wown_recv, w_sem,
            o_send, o_recv, res_sem, out_sem):
    y, d = lax.axis_index("dp"), lax.axis_index("sp")
    c, chip = lax.rem(d, 2), lax.div(d, 2)
    sib = d + 1 - 2 * c
    far = 2 * (1 - chip)
    par = far + c
    to_y, to_sib = {"dp": 1 - y}, {"sp": sib}

    def at(i, n, unit=None):
        return pl.ds(pl.multiple_of(i, unit or n), n)

    def remote(src, dst, send, recv, device):
        return pltpu.make_async_remote_copy(src_ref=src, dst_ref=dst, send_sem=send, recv_sem=recv, device_id=device, device_id_type=MESH)

    def arrived(ref, send, recv, device):
        remote(ref, ref, send, recv, device).wait_recv()

    def source(item, j, core, rows):
        if item == 0:
            return wk_ref.at[rows, at(core * 256, 256)]
        if item == 1:
            return wv_ref.at[rows, at(core * 256, 256)]
        return wq_ref.at[rows, at(core * 2048 + j * COLS, COLS)]

    def place(item, j, rows):
        return wq_s.at[j, rows, :] if item == 2 else pool_s.at[rows, pl.ds(item * 256, 256)]

    def parts(item):
        return (0, 1) if item == 2 else (0,)

    def sem(item, j, p):
        return 2 + 2 * j + p if item == 2 else item

    def rows_of(item, device, half, p):
        n = PART if item == 2 else HALF
        return at(device * OWN + half * HALF + p * n, n)

    def x_copy(item, j, p, t):
        n = sem(item, j, p)
        return remote(source(item, j, t, rows_of(item, 0, y, p)), place(item, j, rows_of(item, d, y, p)), x_send.at[n, t], x_recv.at[n, c], {"sp": far + t})

    def send_x(item, j=0):
        for p in parts(item):
            for t in range(2):
                x_copy(item, j, p, t).start()

    def y_copy(item, j, p, s):
        n, here = sem(item, j, p), place(item, j, rows_of(item, far + s, y, p))
        return remote(here, here, y_send.at[n, s], y_recv.at[n, s], to_y)

    def hand_on(item, j, p):
        n = sem(item, j, p)
        for s in range(2):
            arrived(place(item, j, rows_of(item, far + s, y, p)), x_send.at[n, s], x_recv.at[n, s], {"sp": far + s})
            y_copy(item, j, p, s).start()

    def c_copy(item, j=0):
        n = sem(item, j, 0)
        return remote(source(item, j, 1 - c, pl.ds(0, OWN)), place(item, j, at(d * OWN, OWN)), c_send.at[n], c_recv.at[n], to_sib)

    def own_copy(item, j=0):
        return pltpu.make_async_copy(source(item, j, c, pl.ds(0, OWN)), place(item, j, at(d * OWN, OWN)), own_sem.at[sem(item, j, 0)])

    def near_there(item, j=0):
        n = sem(item, j, 0)
        own_copy(item, j).wait()
        arrived(place(item, j, at(sib * OWN, OWN)), c_send.at[n], c_recv.at[n], to_sib)

    def far_there(item, j=0):
        for p in parts(item):
            n = sem(item, j, p)
            for s in range(2):
                arrived(place(item, j, rows_of(item, far + s, 1 - y, p)), y_send.at[n, s], y_recv.at[n, s], to_y)

    def sent(item, j=0):
        c_copy(item, j).wait_send()
        for p in parts(item):
            for s in range(2):
                x_copy(item, j, p, s).wait_send()
                y_copy(item, j, p, s).wait_send()

    def cols_of(n):
        return at(n * COLS, COLS)

    def wo_x(n):
        return remote(wo_ref.at[at(y * HALF, HALF), cols_of(n)], wo_far.at[at(d * OWN + y * HALF, HALF), cols_of(n)], wx_send.at[n], wx_recv.at[n], {"sp": par})

    def wo_rows(owner, half, n):
        return wo_far.at[at(owner * OWN + half * HALF, HALF), cols_of(n)]

    def wo_y(n):
        return remote(wo_rows(par, y, n), wo_rows(par, y, n), wy_send.at[n], wy_recv.at[n], to_y)

    def wo_c(n, by_y):
        here = wo_rows(par, 1 - y if by_y else y, n)
        return remote(here, here, wc_send.at[by_y, n], wc_recv.at[by_y, n], to_sib)

    def wo_hand_x(n):
        arrived(wo_rows(par, y, n), wx_send.at[n], wx_recv.at[n], {"sp": par})
        wo_y(n).start()
        wo_c(n, 0).start()

    def wo_hand_y(n):
        arrived(wo_rows(par, 1 - y, n), wy_send.at[n], wy_recv.at[n], to_y)
        wo_c(n, 1).start()

    wo_own = remote(wo_ref, wo_far.at[at(d * OWN, OWN), :], wown_send, wown_recv, to_sib)

    def wo_loads(n):
        slot = lax.rem(n, PIECES)
        return [
            pltpu.make_async_copy(wo_ref.at[:, cols_of(n)], wq_s.at[slot, at(d * OWN, OWN), :], w_sem.at[slot, 0]),
            pltpu.make_async_copy(wo_far.at[at(sib * OWN, OWN), cols_of(n)], wq_s.at[slot, at(sib * OWN, OWN), :], w_sem.at[slot, 1]),
            pltpu.make_async_copy(wo_far.at[at(far * OWN, CHIP), cols_of(n)], wq_s.at[slot, at(far * OWN, CHIP), :], w_sem.at[slot, 2]),
        ]

    def wo_load(n):
        for by_y in range(2):
            arrived(wo_rows(far + 1 - c, 1 - y if by_y else y, n), wc_send.at[by_y, n], wc_recv.at[by_y, n], to_sib)
        for copy in wo_loads(n):
            copy.start()

    barrier = pltpu.get_barrier_semaphore()
    for device in (to_sib, {"sp": far}, {"sp": far + 1}, to_y):
        pl.semaphore_signal(barrier, inc=1, device_id=device, device_id_type=MESH)
    tokens = pltpu.make_async_copy(x_ref, a_s.at[at(c * OWN, OWN), :], tok_sem)
    tokens.start()
    pl.semaphore_wait(barrier, 4)
    send_x(0)
    send_x(1)
    send_x(2, 0)
    send_x(2, 1)
    to_other = remote(x_ref, a_s.at[at(c * OWN, OWN), :], tok_send, tok_recv, to_sib)
    to_other.start()
    for item in range(2):
        c_copy(item).start()
        own_copy(item).start()
    for j in range(PIECES):
        c_copy(2, j).start()
        own_copy(2, j).start()
    wo_own.start()
    for g in range(2):
        v_s[g, HEAD:, :] = jnp.ones((16, 2 * CHIP), jnp.bfloat16)

    def norm(first):
        @pl.loop(0, OWN // 128)
        def _(i):
            rows = at(first + i * 128, 128)
            wide = a_s[rows, :].astype(jnp.float32)
            scale = lax.rsqrt(jnp.mean(wide * wide, -1, keepdims=True) + 1e-6)
            a_s[rows, :] = (wide * scale * gain_ref[...].astype(jnp.float32)).astype(jnp.bfloat16)

    tokens.wait()
    norm(c * OWN)
    hand_on(0, 0, 0)
    arrived(a_s.at[at((1 - c) * OWN, OWN), :], tok_send, tok_recv, to_sib)
    norm((1 - c) * OWN)
    hand_on(1, 0, 0)

    def turn(t, m):
        rows = at(m * BLOCK, BLOCK)
        return (t * cos_ref[rows, :] + pltpu.roll(t, HEAD // 2, 1) * sin_ref[rows, :]).astype(jnp.bfloat16)

    near_there(0)
    far_there(0)

    @pl.loop(0, BLOCKS)
    def _(m):
        t = _dot(a_s[at(m * BLOCK, BLOCK), :], pool_s[:, :256], 1, 0).astype(jnp.bfloat16).astype(jnp.float32)
        for g in range(2):
            k_s[g, at(chip * CHIP + m * BLOCK, BLOCK), :] = turn(t[:, g * HEAD : (g + 1) * HEAD], m)

    hand_on(2, 0, 0)
    near_there(1)
    far_there(1)

    @pl.loop(0, BLOCKS)
    def _(m):
        t = _dot(a_s[at(m * BLOCK, BLOCK), :], pool_s[:, 256:], 1, 0)
        for g in range(2):
            v_s[g, :HEAD, at(chip * CHIP + m * BLOCK, BLOCK)] = t[:, g * HEAD : (g + 1) * HEAD].T.astype(jnp.bfloat16)

    def kv_copies(g, kb):
        keys = at(kb * BLOCK, BLOCK)
        return [
            remote(here, here, kv_send.at[g, kb, i], kv_recv.at[g, kb, i], {"sp": c + 2})
            for i, here in enumerate((k_s.at[g, keys, :], v_s.at[g, pl.ds(0, HEAD), keys]))
        ]

    def kv_go(g):
        @pl.when(chip == 0)
        def _():
            for kb in range(BLOCKS):
                for copy in kv_copies(g, kb):
                    copy.start()

    kv_go(0)
    send_x(2, 2)
    kv_go(1)
    send_x(2, 3)
    for n in range(WO):
        wo_x(n).start()
    hand_on(2, 0, 1)

    near_there(2, 0)

    @pl.loop(0, BLOCKS)
    def _(m):
        t = _dot(a_s[at(m * BLOCK, BLOCK), at(chip * CHIP, CHIP)], wq_s[0, at(chip * CHIP, CHIP), :], 1, 0)
        for i in range(HEADS):
            mix_s[m, i, :HEAD, :] = t[i * HEAD : (i + 1) * HEAD, :]

    for item in range(2):
        sent(item)

    def block(g, qb, kb, first=False):
        keys = k_s[g, at(kb * BLOCK, BLOCK), :]
        values = v_s[g, :, at(kb * BLOCK, BLOCK)]
        scores = [_dot(keys, pool_s[at(qb * BLOCK, BLOCK), h * HEAD : (h + 1) * HEAD], 1, 1) for h in range(HEADS)]
        if first:
            seen = lax.broadcasted_iota(jnp.int32, (BLOCK, BLOCK), 0) <= lax.broadcasted_iota(jnp.int32, (BLOCK, BLOCK), 1)
        weights, keeps = [], []
        for h, s in enumerate(scores):
            if first:
                s = jnp.where(seen, s, HIDDEN)
                top = s.max(axis=0, keepdims=True)
            else:
                old = top_s[qb, h : h + 1, :]
                top = jnp.maximum(old, s.max(axis=0, keepdims=True))
                keeps.append(jnp.exp2((old - top) * E))
            top_s[qb, h : h + 1, :] = top
            weights.append(jnp.exp2((s - top) * E).astype(jnp.bfloat16))
        for h, p in enumerate(weights):
            new = _dot(values, p, 1, 0)
            mix_s[qb, h] = new if first else mix_s[qb, h] * keeps[h] + new

    def away(j):
        here = pool_s.at[at(CHIP + lax.rem(j, 2) * OWN, OWN), :]
        return remote(here, o_s.at[:, at(c * 2048 + j * COLS, COLS)], o_send.at[j], o_recv.at[j], to_sib)

    residual = pltpu.make_async_copy(x_ref, a_s.at[pl.ds(0, OWN), :], res_sem)
    hand = {"x": wo_hand_x, "y": wo_hand_y}

    def events(j, point, table):
        for (when, place_), todo in table.items():
            if place_ == point:
                @pl.when(j == when)
                def _():
                    for kind, n in todo:
                        hand[kind](n)

    @pl.loop(0, PIECES)
    def _(j):
        g = lax.div(j, 2)
        events(j, "start", EVENTS)

        def queries(m, t):
            t = t.astype(jnp.bfloat16).astype(jnp.float32)
            for h in range(HEADS):
                pool_s[at(m * BLOCK, BLOCK), h * HEAD : (h + 1) * HEAD] = turn(t[:, h * HEAD : (h + 1) * HEAD], m)

        @pl.when(j == 0)
        def _():
            far_there(2, 0)

            @pl.loop(0, BLOCKS)
            def _(m):
                t = _dot(a_s[at(m * BLOCK, BLOCK), at((1 - chip) * CHIP, CHIP)], wq_s[0, at((1 - chip) * CHIP, CHIP), :], 1, 0)
                queries(m, t + jnp.concatenate([mix_s[m, i, :HEAD, :] for i in range(HEADS)], 0))

        @pl.when(j > 0)
        def _():
            near_there(2, j)
            far_there(2, j)

            @pl.loop(0, BLOCKS)
            def _(m):
                queries(m, _dot(a_s[at(m * BLOCK, BLOCK), :], wq_s[j], 1, 0))

        @pl.when((j == 1) | (j == 2))
        def _():
            for p in range(2):
                hand_on(2, j + 1, p)

        @pl.when(j == PIECES - 1)
        def _():
            residual.start()

        events(j, "pre", EVENTS)

        @pl.loop(0, BLOCKS)
        def _(qb):
            block(g, qb, chip * BLOCKS + qb, True)
            lax.fori_loop(0, qb, lambda i, _: block(g, qb, chip * BLOCKS + i), None)

        @pl.when(j == 0)
        def _():
            for p in range(2):
                hand_on(2, 1, p)

        @pl.when(j >= 2)
        def _():
            away(j - 2).wait_send()

        @pl.loop(0, BLOCKS)
        def _(kb):
            for k in range(BLOCKS):
                @pl.when(kb == k)
                def _():
                    events(j, k, EVENTS)

            @pl.when((chip == 1) & (lax.rem(j, 2) == 0))
            def _():
                for copy in kv_copies(g, kb):
                    copy.wait_recv()

            lax.fori_loop(0, chip * BLOCKS, lambda qb, _: block(g, qb, kb), None)

        def finish(mine):
            core = c if mine else 1 - c

            @pl.loop(0, BLOCKS // 2)
            def _(i):
                qb = core * 2 + i
                for h in range(HEADS):
                    out = (mix_s[qb, h, :HEAD, :] * (1 / mix_s[qb, h, HEAD : HEAD + 1, :])).T.astype(jnp.bfloat16)
                    if mine:
                        o_s[at(i * BLOCK, BLOCK), at(c * 2048 + j * COLS + h * HEAD, HEAD)] = out
                    else:
                        pool_s[at(CHIP + lax.rem(j, 2) * OWN + i * BLOCK, BLOCK), h * HEAD : (h + 1) * HEAD] = out

        finish(False)
        away(j).start()
        finish(True)

    for j in range(PIECES):
        sent(2, j)
    arrived(wo_far.at[at(sib * OWN, OWN), :], wown_send, wown_recv, to_sib)
    wo_load(0)
    wo_load(1)
    residual.wait()
    for j in range(PIECES):
        arrived(o_s.at[:, at((1 - c) * 2048 + j * COLS, COLS)], o_send.at[j], o_recv.at[j], to_sib)

    def out_copy(n):
        return pltpu.make_async_copy(pool_s.at[at(lax.rem(n, 2) * OWN, OWN), :], y_ref.at[:, cols_of(n)], out_sem.at[lax.rem(n, 2)])

    @pl.loop(0, WO)
    def _(n):
        events(n, "out", EVENTS)

        @pl.when(n < WO - 2)
        def _():
            wo_load(n + 2)

        for copy in wo_loads(n):
            copy.wait()

        @pl.when(n >= 2)
        def _():
            out_copy(n - 2).wait()

        slot = lax.rem(n, PIECES)

        @pl.loop(0, OWN // BLOCK)
        def _(m):
            rows = at(m * BLOCK, BLOCK)
            t = a_s[rows, cols_of(n)].astype(jnp.float32) + _dot(o_s[rows, :], wq_s[slot], 1, 0)
            pool_s[at(lax.rem(n, 2) * OWN + m * BLOCK, BLOCK), :] = t.astype(jnp.bfloat16)

        out_copy(n).start()

    for n in range(WO - 2, WO):
        out_copy(n).wait()
    for j in range(2, PIECES):
        away(j).wait_send()

    @pl.when(chip == 0)
    def _():
        for g in range(2):
            for kb in range(BLOCKS):
                for copy in kv_copies(g, kb):
                    copy.wait_send()

    to_other.wait_send()
    wo_own.wait_send()
    for n in range(WO):
        wo_x(n).wait_send()
        wo_y(n).wait_send()
        for by_y in range(2):
            wo_c(n, by_y).wait_send()


EVENTS = {
    (2, 0): [("x", 0)],
    (2, 2): [("x", 1)],
    (2, 3): [("y", 0)],
    (3, "start"): [("x", 2)],
    (3, "pre"): [("y", 1), ("x", 3)],
    (3, 0): [("y", 2), ("x", 4), ("y", 3)],
    (3, 1): [("x", 5)],
    (3, 3): [("x", 6), ("y", 4)],
    (0, "out"): [("y", 5)],
    (1, "out"): [("x", 7)],
    (2, "out"): [("y", 6)],
    (4, "out"): [("y", 7)],
}


def solution(mesh):
    dma = pltpu.SemaphoreType.DMA
    bf16, f32 = jnp.bfloat16, jnp.float32
    anywhere, vmem = pl.BlockSpec(memory_space=pl.ANY), pl.BlockSpec(memory_space=pltpu.VMEM)
    fused = pl.pallas_call(
        _kernel,
        in_specs=[anywhere, vmem, vmem, vmem, anywhere, anywhere, anywhere, anywhere],
        out_specs=[anywhere, anywhere],
        out_shape=[jax.ShapeDtypeStruct((OWN, D), bf16), jax.ShapeDtypeStruct((D, D), bf16)],
        scratch_shapes=[
            pltpu.VMEM((CHIP, D), bf16),
            pltpu.VMEM((PIECES, D, COLS), bf16),
            pltpu.VMEM((D, COLS), bf16),
            pltpu.VMEM((2, 2 * CHIP, HEAD), bf16),
            pltpu.VMEM((2, HEAD + 16, 2 * CHIP), bf16),
            pltpu.VMEM((BLOCKS, HEADS, HEAD + 16, BLOCK), f32),
            pltpu.VMEM((BLOCKS, HEADS, BLOCK), f32),
            pltpu.VMEM((OWN, D), bf16),
            dma((10, 2)), dma((10, 2)), dma((10, 2)), dma((10, 2)), dma((10,)), dma((10,)), dma((10,)), dma, dma, dma,
            dma((2, BLOCKS, 2)), dma((2, BLOCKS, 2)), dma((WO,)), dma((WO,)), dma((WO,)), dma((WO,)), dma((2, WO)), dma((2, WO)), dma, dma,
            dma((PIECES, 3)), dma((PIECES,)), dma((PIECES,)), dma, dma((2,)),
        ],
        compiler_params=pltpu.CompilerParams(collective_id=0, has_side_effects=True, vmem_limit_bytes=67043328),
        cost_estimate=pl.CostEstimate(flops=140 * 10**9, transcendentals=10**8, bytes_accessed=10**8),
    )

    def step(x, gain, wq, wk, wv, wo):
        half = HEAD // 2
        place = lax.div(lax.axis_index("sp"), 2) * CHIP + jnp.arange(CHIP)
        angle = place.astype(f32)[:, None] * THETA ** (-jnp.arange(half, dtype=f32) / half)
        cos, sin = jnp.cos(angle), jnp.sin(angle)
        cos, sin = jnp.concatenate([cos, cos], -1), jnp.concatenate([-sin, sin], -1)
        return fused(x, gain[None], cos, sin, wq, wk, wv, wo)[0]

    tokens, whole = P(("dp", "sp"), None), P("sp", None)
    return jax.shard_map(
        step,
        mesh=mesh,
        in_specs=(tokens, P(None), whole, whole, whole, whole),
        out_specs=tokens,
        check_vma=False,
    )
```

```python
import jax
import jax.numpy as jnp
import numpy as np
from jax import lax
from jax.experimental import pallas as pl
from jax.experimental.pallas import tpu as pltpu
from jax.sharding import PartitionSpec as P

HEAD = 128
THETA = 10000
LOG2E = 1.4426950408889634
HIDDEN = -2e30
OWN = 1024
D = 4096
CHIP = 2 * OWN
HALF = OWN // 2
COLS = 512
PIECES = 4
BLOCK = 512
BLOCKS = CHIP // BLOCK
HEADS = COLS // HEAD
MESH = pl.DeviceIdType.MESH
E = HEAD**-0.5 * LOG2E
WO = D // COLS
PART = HALF // 2


def _dot(a, b, ca, cb):
    return lax.dot_general(a, b, (((ca,), (cb,)), ((), ())), preferred_element_type=jnp.float32)


def _kernel(x_ref, gain_ref, turns_ref, wq_ref, wk_ref, wv_ref, wo_ref, y_ref, wo_far, part_ref,
            a_s, wq_s, pool_s, k_s, v_s, mix_s, top_s, o_s, cos_s, sin_s, gain_s,
            x_send, x_recv, y_send, y_recv, c_send, c_recv, own_sem, tok_sem, tok_send, tok_recv,
            kv_send, kv_recv, wx_send, wx_recv, wy_send, wy_recv, wc_send, wc_recv, wown_send, wown_recv, w_sem,
            o_send, o_recv, res_sem, out_sem, part_sem):
    y, d = lax.axis_index("dp"), lax.axis_index("sp")
    c, chip = lax.rem(d, 2), lax.div(d, 2)
    sib = d + 1 - 2 * c
    far = 2 * (1 - chip)
    par = far + c
    to_y, to_sib = {"dp": 1 - y}, {"sp": sib}

    def at(i, n, unit=None):
        return pl.ds(pl.multiple_of(i, unit or n), n)

    def remote(src, dst, send, recv, device):
        return pltpu.make_async_remote_copy(src_ref=src, dst_ref=dst, send_sem=send, recv_sem=recv, device_id=device, device_id_type=MESH)

    def arrived(ref, send, recv, device):
        remote(ref, ref, send, recv, device).wait_recv()

    def source(item, j, core, rows):
        if item == 0:
            return wk_ref.at[rows, at(core * 256, 256)]
        if item == 1:
            return wv_ref.at[rows, at(core * 256, 256)]
        return wq_ref.at[rows, at(core * 2048 + j * COLS, COLS)]

    def place(item, j, rows):
        return wq_s.at[j, rows, :] if item == 2 else pool_s.at[rows, pl.ds(item * 256, 256)]

    def parts(item):
        return (0, 1) if item == 2 else (0,)

    def sem(item, j, p):
        return 2 + 2 * j + p if item == 2 else item

    def rows_of(item, device, half, p):
        n = PART if item == 2 else HALF
        return at(device * OWN + half * HALF + p * n, n)

    def x_copy(item, j, p, t):
        n = sem(item, j, p)
        return remote(source(item, j, t, rows_of(item, 0, y, p)), place(item, j, rows_of(item, d, y, p)), x_send.at[n, t], x_recv.at[n, c], {"sp": far + t})

    def send_x(item, j=0):
        for p in parts(item):
            for t in range(2):
                x_copy(item, j, p, t).start()

    def y_copy(item, j, p, s):
        n, here = sem(item, j, p), place(item, j, rows_of(item, far + s, y, p))
        return remote(here, here, y_send.at[n, s], y_recv.at[n, s], to_y)

    def hand_on(item, j, p):
        n = sem(item, j, p)
        for s in range(2):
            arrived(place(item, j, rows_of(item, far + s, y, p)), x_send.at[n, s], x_recv.at[n, s], {"sp": far + s})
            y_copy(item, j, p, s).start()

    def c_copy(item, j=0):
        n = sem(item, j, 0)
        return remote(source(item, j, 1 - c, pl.ds(0, OWN)), place(item, j, at(d * OWN, OWN)), c_send.at[n], c_recv.at[n], to_sib)

    def own_copy(item, j=0):
        return pltpu.make_async_copy(source(item, j, c, pl.ds(0, OWN)), place(item, j, at(d * OWN, OWN)), own_sem.at[sem(item, j, 0)])

    def near_there(item, j=0):
        n = sem(item, j, 0)
        own_copy(item, j).wait()
        arrived(place(item, j, at(sib * OWN, OWN)), c_send.at[n], c_recv.at[n], to_sib)

    def far_there(item, j=0):
        for p in parts(item):
            n = sem(item, j, p)
            for s in range(2):
                arrived(place(item, j, rows_of(item, far + s, 1 - y, p)), y_send.at[n, s], y_recv.at[n, s], to_y)

    def sent(item, j=0):
        c_copy(item, j).wait_send()
        for p in parts(item):
            for s in range(2):
                x_copy(item, j, p, s).wait_send()
                y_copy(item, j, p, s).wait_send()

    def cols_of(n):
        return at(n * COLS, COLS)

    def wo_x(n):
        return remote(wo_ref.at[at(y * HALF, HALF), cols_of(n)], wo_far.at[at(d * OWN + y * HALF, HALF), cols_of(n)], wx_send.at[n], wx_recv.at[n], {"sp": par})

    def wo_rows(owner, half, n):
        return wo_far.at[at(owner * OWN + half * HALF, HALF), cols_of(n)]

    def wo_y(n):
        return remote(wo_rows(par, y, n), wo_rows(par, y, n), wy_send.at[n], wy_recv.at[n], to_y)

    def wo_c(n, by_y):
        here = wo_rows(par, 1 - y if by_y else y, n)
        return remote(here, here, wc_send.at[by_y, n], wc_recv.at[by_y, n], to_sib)

    def wo_hand_x(n):
        arrived(wo_rows(par, y, n), wx_send.at[n], wx_recv.at[n], {"sp": par})
        wo_y(n).start()
        wo_c(n, 0).start()

    def wo_hand_y(n):
        arrived(wo_rows(par, 1 - y, n), wy_send.at[n], wy_recv.at[n], to_y)
        wo_c(n, 1).start()

    wo_own = remote(wo_ref, wo_far.at[at(d * OWN, OWN), :], wown_send, wown_recv, to_sib)

    def wo_loads(n):
        slot = lax.rem(n, PIECES)
        return [
            pltpu.make_async_copy(wo_ref.at[:, cols_of(n)], wq_s.at[slot, at(d * OWN, OWN), :], w_sem.at[slot, 0]),
            pltpu.make_async_copy(wo_far.at[at(sib * OWN, OWN), cols_of(n)], wq_s.at[slot, at(sib * OWN, OWN), :], w_sem.at[slot, 1]),
            pltpu.make_async_copy(wo_far.at[at(far * OWN, CHIP), cols_of(n)], wq_s.at[slot, at(far * OWN, CHIP), :], w_sem.at[slot, 2]),
        ]

    def wo_load(n):
        for by_y in range(2):
            arrived(wo_rows(far + 1 - c, 1 - y if by_y else y, n), wc_send.at[by_y, n], wc_recv.at[by_y, n], to_sib)
        for copy in wo_loads(n):
            copy.start()

    barrier = pltpu.get_barrier_semaphore()
    for device in (to_sib, {"sp": far}, {"sp": far + 1}, to_y):
        pl.semaphore_signal(barrier, inc=1, device_id=device, device_id_type=MESH)
    tokens = pltpu.make_async_copy(x_ref, a_s.at[at(c * OWN, OWN), :], tok_sem)
    tokens.start()
    pl.semaphore_wait(barrier, 4)
    send_x(0)
    send_x(1)
    send_x(2, 0)
    send_x(2, 1)
    to_other = remote(x_ref, a_s.at[at(c * OWN, OWN), :], tok_send, tok_recv, to_sib)
    to_other.start()
    for item in range(2):
        c_copy(item).start()
        own_copy(item).start()
    for j in range(PIECES):
        c_copy(2, j).start()
        own_copy(2, j).start()
    wo_own.start()
    for g in range(2):
        v_s[g, HEAD:, :] = jnp.ones((16, 2 * CHIP), jnp.bfloat16)

    @pl.loop(0, CHIP // 64)
    def _(i):
        h = pl.ds(chip * (CHIP // 64) + i, 1)
        ch, sh, cl, sl = turns_ref[0, h, :], turns_ref[1, h, :], turns_ref[2], turns_ref[3]
        cos_s[at(i * 64, 64), :] = ch * cl - sh * sl
        sin_s[at(i * 64, 64), :] = sh * cl + ch * sl

    gain_s[...] = gain_ref[...].astype(jnp.float32).reshape(1, D)

    def norm(first):
        @pl.loop(0, OWN // 128)
        def _(i):
            rows = at(first + i * 128, 128)
            wide = a_s[rows, :].astype(jnp.float32)
            scale = lax.rsqrt(jnp.mean(wide * wide, -1, keepdims=True) + 1e-6)
            a_s[rows, :] = (wide * scale * gain_s[...]).astype(jnp.bfloat16)

    tokens.wait()
    norm(c * OWN)
    hand_on(0, 0, 0)
    arrived(a_s.at[at((1 - c) * OWN, OWN), :], tok_send, tok_recv, to_sib)
    norm((1 - c) * OWN)
    hand_on(1, 0, 0)

    def turn(t, m):
        rows = at(m * BLOCK, BLOCK)
        return (t * cos_s[rows, :] + pltpu.roll(t, HEAD // 2, 1) * sin_s[rows, :]).astype(jnp.bfloat16)

    near_there(0)
    far_there(0)

    @pl.loop(0, BLOCKS)
    def _(m):
        t = _dot(a_s[at(m * BLOCK, BLOCK), :], pool_s[:, :256], 1, 0).astype(jnp.bfloat16).astype(jnp.float32)
        for g in range(2):
            k_s[g, at(chip * CHIP + m * BLOCK, BLOCK), :] = turn(t[:, g * HEAD : (g + 1) * HEAD], m)

    def part_copy(j, m, back):
        here, there = mix_s.at[m, :, pl.ds(0, HEAD), :], part_ref.at[j - 1, m]
        return pltpu.make_async_copy(there, here, part_sem.at[m]) if back else pltpu.make_async_copy(here, there, part_sem.at[m])

    def near_queries(j):
        near_there(2, j)

        @pl.loop(0, BLOCKS)
        def _(m):
            if j < PIECES - 1:
                part_copy(j + 1, m, False).wait()
            t = _dot(a_s[at(m * BLOCK, BLOCK), at(chip * CHIP, CHIP)], wq_s[j, at(chip * CHIP, CHIP), :], 1, 0)
            for i in range(HEADS):
                mix_s[m, i, :HEAD, :] = t[i * HEAD : (i + 1) * HEAD, :]
            if j:
                part_copy(j, m, False).start()

    near_queries(3)
    hand_on(2, 0, 0)
    near_there(1)
    far_there(1)

    @pl.loop(0, BLOCKS)
    def _(m):
        t = _dot(a_s[at(m * BLOCK, BLOCK), :], pool_s[:, 256:], 1, 0)
        for g in range(2):
            v_s[g, :HEAD, at(chip * CHIP + m * BLOCK, BLOCK)] = t[:, g * HEAD : (g + 1) * HEAD].T.astype(jnp.bfloat16)

    def kv_copies(g, kb):
        keys = at(kb * BLOCK, BLOCK)
        return [
            remote(here, here, kv_send.at[g, kb, i], kv_recv.at[g, kb, i], {"sp": c + 2})
            for i, here in enumerate((k_s.at[g, keys, :], v_s.at[g, pl.ds(0, HEAD), keys]))
        ]

    def kv_go(g):
        @pl.when(chip == 0)
        def _():
            for kb in range(BLOCKS):
                for copy in kv_copies(g, kb):
                    copy.start()

    kv_go(0)
    send_x(2, 2)
    kv_go(1)
    send_x(2, 3)
    for n in range(WO):
        wo_x(n).start()
    near_queries(2)
    hand_on(2, 0, 1)
    near_queries(1)
    near_queries(0)
    for item in range(2):
        sent(item)

    def block(g, qb, kb, first=False):
        keys = k_s[g, at(kb * BLOCK, BLOCK), :]
        values = v_s[g, :, at(kb * BLOCK, BLOCK)]
        scores = [_dot(keys, pool_s[at(qb * BLOCK, BLOCK), h * HEAD : (h + 1) * HEAD], 1, 1) for h in range(HEADS)]
        if first:
            seen = lax.broadcasted_iota(jnp.int32, (BLOCK, BLOCK), 0) <= lax.broadcasted_iota(jnp.int32, (BLOCK, BLOCK), 1)
        weights, keeps = [], []
        for h, s in enumerate(scores):
            if first:
                s = jnp.where(seen, s, HIDDEN)
                top = s.max(axis=0, keepdims=True)
            else:
                old = top_s[qb, h : h + 1, :]
                top = jnp.maximum(old, s.max(axis=0, keepdims=True))
                keeps.append(jnp.exp2((old - top) * E))
            top_s[qb, h : h + 1, :] = top
            weights.append(jnp.exp2((s - top) * E).astype(jnp.bfloat16))
        for h, p in enumerate(weights):
            new = _dot(values, p, 1, 0)
            mix_s[qb, h] = new if first else mix_s[qb, h] * keeps[h] + new

    def away(j):
        here = pool_s.at[at(CHIP + lax.rem(j, 2) * OWN, OWN), :]
        return remote(here, o_s.at[:, at(c * 2048 + j * COLS, COLS)], o_send.at[j], o_recv.at[j], to_sib)

    residual = pltpu.make_async_copy(x_ref, a_s.at[pl.ds(0, OWN), :], res_sem)
    hand = {"x": wo_hand_x, "y": wo_hand_y}

    def events(j, point, table):
        for (when, place_), todo in table.items():
            if place_ == point:
                @pl.when(j == when)
                def _():
                    for kind, n in todo:
                        hand[kind](n)

    @pl.loop(0, PIECES)
    def _(j):
        g = lax.div(j, 2)
        events(j, "start", EVENTS)

        def queries(m, t):
            t = t.astype(jnp.bfloat16).astype(jnp.float32)
            for h in range(HEADS):
                pool_s[at(m * BLOCK, BLOCK), h * HEAD : (h + 1) * HEAD] = turn(t[:, h * HEAD : (h + 1) * HEAD], m)

        far_there(2, j)

        @pl.loop(0, BLOCKS)
        def _(m):
            @pl.when(j > 0)
            def _():
                part_copy(j, m, True).wait()

            t = _dot(a_s[at(m * BLOCK, BLOCK), at((1 - chip) * CHIP, CHIP)], wq_s[j, at((1 - chip) * CHIP, CHIP), :], 1, 0)
            queries(m, t + jnp.concatenate([mix_s[m, i, :HEAD, :] for i in range(HEADS)], 0))

        @pl.when(j == PIECES - 1)
        def _():
            residual.start()

        @pl.loop(0, BLOCKS)
        def _(qb):
            for k in range(BLOCKS):
                @pl.when(qb == k)
                def _():
                    events(j, ("own", k), EVENTS)

            block(g, qb, chip * BLOCKS + qb, True)
            lax.fori_loop(0, qb, lambda i, _: block(g, qb, chip * BLOCKS + i), None)

        @pl.when(j < PIECES - 1)
        def _():
            for p in range(2):
                hand_on(2, j + 1, p)

        @pl.when(j >= 2)
        def _():
            away(j - 2).wait_send()

        @pl.loop(0, BLOCKS)
        def _(kb):
            for k in range(BLOCKS):
                @pl.when(kb == k)
                def _():
                    events(j, k, EVENTS)

            @pl.when((chip == 1) & (lax.rem(j, 2) == 0))
            def _():
                for copy in kv_copies(g, kb):
                    copy.wait_recv()

            lax.fori_loop(0, chip * BLOCKS, lambda qb, _: block(g, qb, kb), None)

        def finish(mine):
            core = c if mine else 1 - c

            @pl.loop(0, BLOCKS // 2)
            def _(i):
                qb = core * 2 + i
                for h in range(HEADS):
                    out = (mix_s[qb, h, :HEAD, :] * (1 / mix_s[qb, h, HEAD : HEAD + 1, :])).T.astype(jnp.bfloat16)
                    if mine:
                        o_s[at(i * BLOCK, BLOCK), at(c * 2048 + j * COLS + h * HEAD, HEAD)] = out
                    else:
                        pool_s[at(CHIP + lax.rem(j, 2) * OWN + i * BLOCK, BLOCK), h * HEAD : (h + 1) * HEAD] = out

        finish(False)
        away(j).start()
        finish(True)

        @pl.when(j < PIECES - 1)
        def _():
            for m in range(BLOCKS):
                part_copy(j + 1, m, True).start()

    for j in range(PIECES):
        sent(2, j)
    arrived(wo_far.at[at(sib * OWN, OWN), :], wown_send, wown_recv, to_sib)
    wo_load(0)
    residual.wait()
    for j in range(PIECES):
        arrived(o_s.at[:, at((1 - c) * 2048 + j * COLS, COLS)], o_send.at[j], o_recv.at[j], to_sib)

    def out_copy(n):
        return pltpu.make_async_copy(pool_s.at[at(lax.rem(n, 2) * OWN, OWN), :], y_ref.at[:, cols_of(n)], out_sem.at[lax.rem(n, 2)])

    @pl.loop(0, WO)
    def _(n):
        for copy in wo_loads(n):
            copy.wait()

        @pl.when(n >= 2)
        def _():
            out_copy(n - 2).wait()

        slot = lax.rem(n, PIECES)

        @pl.loop(0, OWN // BLOCK)
        def _(m):
            @pl.when(m == 1)
            def _():
                events(n, "out", EVENTS)

                @pl.when(n < WO - 1)
                def _():
                    wo_load(n + 1)

            rows = at(m * BLOCK, BLOCK)
            t = a_s[rows, cols_of(n)].astype(jnp.float32) + _dot(o_s[rows, :], wq_s[slot], 1, 0)
            pool_s[at(lax.rem(n, 2) * OWN + m * BLOCK, BLOCK), :] = t.astype(jnp.bfloat16)

        out_copy(n).start()

    for n in range(WO - 2, WO):
        out_copy(n).wait()
    for j in range(2, PIECES):
        away(j).wait_send()

    @pl.when(chip == 0)
    def _():
        for g in range(2):
            for kb in range(BLOCKS):
                for copy in kv_copies(g, kb):
                    copy.wait_send()

    to_other.wait_send()
    wo_own.wait_send()
    for n in range(WO):
        wo_x(n).wait_send()
        wo_y(n).wait_send()
        for by_y in range(2):
            wo_c(n, by_y).wait_send()


EVENTS = {
    (2, 2): [("x", 0)],
    (3, "start"): [("x", 1)],
    (3, ("own", 0)): [("y", 0)],
    (3, ("own", 2)): [("x", 2)],
    (3, ("own", 3)): [("y", 1)],
    (3, 0): [("x", 3)],
    (3, 1): [("y", 2)],
    (3, 2): [("x", 4)],
    (3, 3): [("y", 3)],
    (0, "out"): [("x", 5), ("y", 4)],
    (2, "out"): [("x", 6)],
    (3, "out"): [("y", 5)],
    (4, "out"): [("x", 7)],
    (5, "out"): [("y", 6)],
    (6, "out"): [("y", 7)],
}


def solution(mesh):
    dma = pltpu.SemaphoreType.DMA
    bf16, f32 = jnp.bfloat16, jnp.float32
    anywhere, vmem = pl.BlockSpec(memory_space=pl.ANY), pl.BlockSpec(memory_space=pltpu.VMEM)
    fused = pl.pallas_call(
        _kernel,
        in_specs=[anywhere, vmem, vmem, anywhere, anywhere, anywhere, anywhere],
        out_specs=[anywhere, anywhere, anywhere],
        out_shape=[jax.ShapeDtypeStruct((OWN, D), bf16), jax.ShapeDtypeStruct((D, D), bf16),
                   jax.ShapeDtypeStruct((PIECES - 1, BLOCKS, HEADS, HEAD, COLS), f32)],
        scratch_shapes=[
            pltpu.VMEM((CHIP, D), bf16),
            pltpu.VMEM((PIECES, D, COLS), bf16),
            pltpu.VMEM((D, COLS), bf16),
            pltpu.VMEM((2, 2 * CHIP, HEAD), bf16),
            pltpu.VMEM((2, HEAD + 16, 2 * CHIP), bf16),
            pltpu.VMEM((BLOCKS, HEADS, HEAD + 16, BLOCK), f32),
            pltpu.VMEM((BLOCKS, HEADS, BLOCK), f32),
            pltpu.VMEM((OWN, D), bf16),
            pltpu.VMEM((CHIP, HEAD), f32),
            pltpu.VMEM((CHIP, HEAD), f32),
            pltpu.VMEM((1, D), f32),
            dma((10, 2)), dma((10, 2)), dma((10, 2)), dma((10, 2)), dma((10,)), dma((10,)), dma((10,)), dma, dma, dma,
            dma((2, BLOCKS, 2)), dma((2, BLOCKS, 2)), dma((WO,)), dma((WO,)), dma((WO,)), dma((WO,)), dma((2, WO)), dma((2, WO)), dma, dma,
            dma((PIECES, 3)), dma((PIECES,)), dma((PIECES,)), dma, dma((2,)), dma((BLOCKS,)),
        ],
        compiler_params=pltpu.CompilerParams(collective_id=0, has_side_effects=True, vmem_limit_bytes=67043328),
        cost_estimate=pl.CostEstimate(flops=140 * 10**9, transcendentals=10**8, bytes_accessed=10**8),
    )

    freq = np.tile(float(THETA) ** (-np.arange(HEAD // 2) / (HEAD // 2)), 2)
    sign = np.where(np.arange(HEAD) < HEAD // 2, -1.0, 1.0)
    angles = [np.arange(64)[:, None] * n * freq for n in (64, 1)]
    turns = np.stack([f(t) for t in angles for f in (np.cos, lambda t: sign * np.sin(t))]).astype(np.float32)

    def step(x, gain, wq, wk, wv, wo):
        return fused(x, gain, turns, wq, wk, wv, wo)[0]

    tokens, whole = P(("dp", "sp"), None), P("sp", None)
    return jax.shard_map(
        step,
        mesh=mesh,
        in_specs=(tokens, P(None), whole, whole, whole, whole),
        out_specs=tokens,
        check_vma=False,
    )
```

```python
import jax
import jax.numpy as jnp
import numpy as np
from jax import lax
from jax.experimental import pallas as pl
from jax.experimental.pallas import tpu as pltpu
from jax.sharding import PartitionSpec as P

HEAD = 128
THETA = 10000
LOG2E = 1.4426950408889634
HIDDEN = -2e30
OWN = 1024
D = 4096
CHIP = 2 * OWN
HALF = OWN // 2
COLS = 512
PIECES = 4
BLOCK = 512
BLOCKS = CHIP // BLOCK
HEADS = COLS // HEAD
MESH = pl.DeviceIdType.MESH
E = HEAD**-0.5 * LOG2E
WCOLS = 256
WO = D // WCOLS
FULL = BLOCKS * (BLOCKS - 1) // 2
STEPS = FULL + BLOCKS * BLOCKS
PART = HALF // 2


def _dot(a, b, ca, cb):
    return lax.dot_general(a, b, (((ca,), (cb,)), ((), ())), preferred_element_type=jnp.float32)


def _kernel(x_ref, gain_ref, turns_ref, wq_ref, wk_ref, wv_ref, wo_ref, y_ref, wo_far, part_ref,
            a_s, wq_s, pool_s, k_s, v_s, mix_s, top_s, s_s, o_s, cos_s, sin_s, gain_s,
            x_send, x_recv, y_send, y_recv, c_send, c_recv, own_sem, tok_sem, tok_send, tok_recv,
            kv_send, kv_recv, wx_send, wx_recv, wy_send, wy_recv, wc_send, wc_recv, wown_send, wown_recv, w_sem,
            o_send, o_recv, res_sem, out_sem, part_sem):
    y, d = lax.axis_index("dp"), lax.axis_index("sp")
    c, chip = lax.rem(d, 2), lax.div(d, 2)
    sib = d + 1 - 2 * c
    far = 2 * (1 - chip)
    par = far + c
    to_y, to_sib = {"dp": 1 - y}, {"sp": sib}

    def at(i, n, unit=None):
        return pl.ds(pl.multiple_of(i, unit or n), n)

    def remote(src, dst, send, recv, device):
        return pltpu.make_async_remote_copy(src_ref=src, dst_ref=dst, send_sem=send, recv_sem=recv, device_id=device, device_id_type=MESH)

    def arrived(ref, send, recv, device):
        remote(ref, ref, send, recv, device).wait_recv()

    def source(item, j, core, rows):
        if item == 0:
            return wk_ref.at[rows, at(core * 256, 256)]
        if item == 1:
            return wv_ref.at[rows, at(core * 256, 256)]
        return wq_ref.at[rows, at(core * 2048 + j * COLS, COLS)]

    def place(item, j, rows):
        return wq_s.at[j, rows, :] if item == 2 else pool_s.at[rows, pl.ds(item * 256, 256)]

    def parts(item):
        return (0, 1) if item == 2 else (0,)

    def sem(item, j, p):
        return 2 + 2 * j + p if item == 2 else item

    def rows_of(item, device, half, p):
        n = PART if item == 2 else HALF
        return at(device * OWN + half * HALF + p * n, n)

    def x_copy(item, j, p, t):
        n = sem(item, j, p)
        return remote(source(item, j, t, rows_of(item, 0, y, p)), place(item, j, rows_of(item, d, y, p)), x_send.at[n, t], x_recv.at[n, c], {"sp": far + t})

    def send_x(item, j=0):
        for p in parts(item):
            for t in range(2):
                x_copy(item, j, p, t).start()

    def y_copy(item, j, p, s):
        n, here = sem(item, j, p), place(item, j, rows_of(item, far + s, y, p))
        return remote(here, here, y_send.at[n, s], y_recv.at[n, s], to_y)

    def hand_on(item, j, p):
        n = sem(item, j, p)
        for s in range(2):
            arrived(place(item, j, rows_of(item, far + s, y, p)), x_send.at[n, s], x_recv.at[n, s], {"sp": far + s})
            y_copy(item, j, p, s).start()

    def c_copy(item, j=0):
        n = sem(item, j, 0)
        return remote(source(item, j, 1 - c, pl.ds(0, OWN)), place(item, j, at(d * OWN, OWN)), c_send.at[n], c_recv.at[n], to_sib)

    def own_copy(item, j=0):
        return pltpu.make_async_copy(source(item, j, c, pl.ds(0, OWN)), place(item, j, at(d * OWN, OWN)), own_sem.at[sem(item, j, 0)])

    def near_there(item, j=0):
        n = sem(item, j, 0)
        own_copy(item, j).wait()
        arrived(place(item, j, at(sib * OWN, OWN)), c_send.at[n], c_recv.at[n], to_sib)

    def far_there(item, j=0):
        for p in parts(item):
            n = sem(item, j, p)
            for s in range(2):
                arrived(place(item, j, rows_of(item, far + s, 1 - y, p)), y_send.at[n, s], y_recv.at[n, s], to_y)

    def sent(item, j=0):
        c_copy(item, j).wait_send()
        for p in parts(item):
            for s in range(2):
                x_copy(item, j, p, s).wait_send()
                y_copy(item, j, p, s).wait_send()

    def cols_of(n):
        return at(n * WCOLS, WCOLS)

    def wo_x(n):
        return remote(wo_ref.at[at(y * HALF, HALF), cols_of(n)], wo_far.at[at(d * OWN + y * HALF, HALF), cols_of(n)], wx_send.at[n], wx_recv.at[n], {"sp": par})

    def wo_rows(owner, half, n):
        return wo_far.at[at(owner * OWN + half * HALF, HALF), cols_of(n)]

    def wo_y(n):
        return remote(wo_rows(par, y, n), wo_rows(par, y, n), wy_send.at[n], wy_recv.at[n], to_y)

    def wo_c(n, by_y):
        here = wo_rows(par, 1 - y if by_y else y, n)
        return remote(here, here, wc_send.at[by_y, n], wc_recv.at[by_y, n], to_sib)

    def wo_hand_x(n):
        arrived(wo_rows(par, y, n), wx_send.at[n], wx_recv.at[n], {"sp": par})
        wo_y(n).start()
        wo_c(n, 0).start()

    def wo_hand_y(n):
        arrived(wo_rows(par, 1 - y, n), wy_send.at[n], wy_recv.at[n], to_y)
        wo_c(n, 1).start()

    wo_own = remote(wo_ref, wo_far.at[at(d * OWN, OWN), :], wown_send, wown_recv, to_sib)

    def wo_loads(n):
        slot = lax.rem(n, PIECES)
        return [
            pltpu.make_async_copy(wo_ref.at[:, cols_of(n)], wq_s.at[slot, at(d * OWN, OWN), pl.ds(0, WCOLS)], w_sem.at[slot, 0]),
            pltpu.make_async_copy(wo_far.at[at(sib * OWN, OWN), cols_of(n)], wq_s.at[slot, at(sib * OWN, OWN), pl.ds(0, WCOLS)], w_sem.at[slot, 1]),
            pltpu.make_async_copy(wo_far.at[at(far * OWN, CHIP), cols_of(n)], wq_s.at[slot, at(far * OWN, CHIP), pl.ds(0, WCOLS)], w_sem.at[slot, 2]),
        ]

    def wo_load(n):
        for by_y in range(2):
            arrived(wo_rows(far + 1 - c, 1 - y if by_y else y, n), wc_send.at[by_y, n], wc_recv.at[by_y, n], to_sib)
        for copy in wo_loads(n):
            copy.start()

    barrier = pltpu.get_barrier_semaphore()
    for device in (to_sib, {"sp": far}, {"sp": far + 1}, to_y):
        pl.semaphore_signal(barrier, inc=1, device_id=device, device_id_type=MESH)
    tokens = pltpu.make_async_copy(x_ref, a_s.at[at(c * OWN, OWN), :], tok_sem)
    tokens.start()
    pl.semaphore_wait(barrier, 4)
    send_x(0)
    send_x(1)
    send_x(2, 0)
    send_x(2, 1)
    to_other = remote(x_ref, a_s.at[at(c * OWN, OWN), :], tok_send, tok_recv, to_sib)
    to_other.start()
    for item in range(2):
        c_copy(item).start()
        own_copy(item).start()
    for j in range(PIECES):
        c_copy(2, j).start()
        own_copy(2, j).start()
    wo_own.start()
    for g in range(2):
        v_s[g, HEAD:, :] = jnp.ones((16, 2 * CHIP), jnp.bfloat16)

    @pl.loop(0, CHIP // 64)
    def _(i):
        h = pl.ds(chip * (CHIP // 64) + i, 1)
        ch, sh, cl, sl = turns_ref[0, h, :], turns_ref[1, h, :], turns_ref[2], turns_ref[3]
        cos_s[at(i * 64, 64), :] = ch * cl - sh * sl
        sin_s[at(i * 64, 64), :] = sh * cl + ch * sl

    gain_s[...] = gain_ref[...].astype(jnp.float32).reshape(1, D)

    def norm(first):
        @pl.loop(0, OWN // 128)
        def _(i):
            rows = at(first + i * 128, 128)
            wide = a_s[rows, :].astype(jnp.float32)
            scale = lax.rsqrt(jnp.mean(wide * wide, -1, keepdims=True) + 1e-6)
            a_s[rows, :] = (wide * scale * gain_s[...]).astype(jnp.bfloat16)

    tokens.wait()
    norm(c * OWN)
    hand_on(0, 0, 0)
    arrived(a_s.at[at((1 - c) * OWN, OWN), :], tok_send, tok_recv, to_sib)
    norm((1 - c) * OWN)
    hand_on(1, 0, 0)

    def turn(t, m):
        rows = at(m * BLOCK, BLOCK)
        return (t * cos_s[rows, :] + pltpu.roll(t, HEAD // 2, 1) * sin_s[rows, :]).astype(jnp.bfloat16)

    near_there(0)
    far_there(0)

    @pl.loop(0, BLOCKS)
    def _(m):
        t = _dot(a_s[at(m * BLOCK, BLOCK), :], pool_s[:, :256], 1, 0).astype(jnp.bfloat16).astype(jnp.float32)
        for g in range(2):
            k_s[g, at(chip * CHIP + m * BLOCK, BLOCK), :] = turn(t[:, g * HEAD : (g + 1) * HEAD], m)

    def part_copy(j, m, back):
        here, there = mix_s.at[m, :, pl.ds(0, HEAD), :], part_ref.at[j - 1, m]
        return pltpu.make_async_copy(there, here, part_sem.at[m]) if back else pltpu.make_async_copy(here, there, part_sem.at[m])

    def near_queries(j):
        near_there(2, j)

        @pl.loop(0, BLOCKS)
        def _(m):
            if j < PIECES - 1:
                part_copy(j + 1, m, False).wait()
            t = _dot(a_s[at(m * BLOCK, BLOCK), at(chip * CHIP, CHIP)], wq_s[j, at(chip * CHIP, CHIP), :], 1, 0)
            for i in range(HEADS):
                mix_s[m, i, :HEAD, :] = t[i * HEAD : (i + 1) * HEAD, :]
            if j:
                part_copy(j, m, False).start()

    near_queries(3)
    hand_on(2, 0, 0)
    near_there(1)
    far_there(1)

    @pl.loop(0, BLOCKS)
    def _(m):
        t = _dot(a_s[at(m * BLOCK, BLOCK), :], pool_s[:, 256:], 1, 0)
        for g in range(2):
            v_s[g, :HEAD, at(chip * CHIP + m * BLOCK, BLOCK)] = t[:, g * HEAD : (g + 1) * HEAD].T.astype(jnp.bfloat16)

    def kv_copies(g, kb):
        keys = at(kb * BLOCK, BLOCK)
        return [
            remote(here, here, kv_send.at[g, kb, i], kv_recv.at[g, kb, i], {"sp": c + 2})
            for i, here in enumerate((k_s.at[g, keys, :], v_s.at[g, pl.ds(0, HEAD), keys]))
        ]

    def kv_go(g):
        @pl.when(chip == 0)
        def _():
            for kb in range(BLOCKS):
                for copy in kv_copies(g, kb):
                    copy.start()

    kv_go(0)
    send_x(2, 2)
    kv_go(1)
    send_x(2, 3)
    for n in range(WO):
        wo_x(n).start()
    near_queries(2)
    hand_on(2, 0, 1)
    near_queries(1)
    near_queries(0)
    for item in range(2):
        sent(item)

    def diagonal(g, qb):
        half = BLOCK // 2
        at_keys = chip * CHIP + qb * BLOCK
        keys, values = k_s[g, at(at_keys, BLOCK), :], v_s[g, :, at(at_keys, BLOCK)]
        seen = lax.broadcasted_iota(jnp.int32, (half, half), 0) <= lax.broadcasted_iota(jnp.int32, (half, half), 1)
        for h in range(HEADS):
            q = pool_s[at(qb * BLOCK, BLOCK), h * HEAD : (h + 1) * HEAD]
            early, late = _dot(keys[:half], q, 1, 1), _dot(keys[half:], q[half:], 1, 1)
            left, late = jnp.where(seen, early[:, :half], HIDDEN), jnp.where(seen, late, HIDDEN)
            right = jnp.concatenate([early[:, half:], late], 0)
            for s, cols, n in ((left, pl.ds(0, half), half), (right, pl.ds(half, half), BLOCK)):
                top = s.max(axis=0, keepdims=True)
                top_s[qb, h : h + 1, cols] = top
                mix_s[qb, h, :, cols] = _dot(values[:, :n], jnp.exp2((s - top) * E).astype(jnp.bfloat16), 1, 0)

    def place_of(t):
        own_qb = 1 + jnp.where(t >= 1, 1, 0) + jnp.where(t >= 3, 1, 0)
        own_kb = t - jnp.where(t >= 1, 1, 0) - jnp.where(t >= 3, 2, 0) + chip * BLOCKS
        return jnp.where(t < FULL, own_qb, lax.rem(t + BLOCKS * BLOCKS - FULL, BLOCKS)), jnp.where(t < FULL, own_kb, lax.div(t - FULL, BLOCKS))

    def score(g, t, h):
        qb, kb = place_of(t)
        s_s[h] = _dot(k_s[g, at(kb * BLOCK, BLOCK), :], pool_s[at(qb * BLOCK, BLOCK), h * HEAD : (h + 1) * HEAD], 1, 1)

    def step(g, t, last):
        qb, kb = place_of(t)
        values = v_s[g, :, at(kb * BLOCK, BLOCK)]
        for h in range(HEADS):
            s = s_s[h]
            old = top_s[qb, h : h + 1, :]
            top = jnp.maximum(old, s.max(axis=0, keepdims=True))
            keep = jnp.exp2((old - top) * E)
            top_s[qb, h : h + 1, :] = top
            p = jnp.exp2((s - top) * E).astype(jnp.bfloat16)
            score(g, jnp.minimum(t + 1, last), h)
            mix_s[qb, h] = mix_s[qb, h] * keep + _dot(values, p, 1, 0)

    def away(j):
        here = pool_s.at[at(CHIP + lax.rem(j, 2) * OWN, OWN), :]
        return remote(here, o_s.at[:, at(c * 2048 + j * COLS, COLS)], o_send.at[j], o_recv.at[j], to_sib)

    residual = pltpu.make_async_copy(x_ref, a_s.at[pl.ds(0, OWN), :], res_sem)
    hand = {"x": wo_hand_x, "y": wo_hand_y}

    def events(j, point, table):
        for (when, place_), todo in table.items():
            if place_ == point:
                @pl.when(j == when)
                def _():
                    for kind, n in todo:
                        hand[kind](n)

    @pl.loop(0, PIECES)
    def _(j):
        g = lax.div(j, 2)
        events(j, "start", EVENTS)

        def queries(m, t):
            t = t.astype(jnp.bfloat16).astype(jnp.float32)
            for h in range(HEADS):
                pool_s[at(m * BLOCK, BLOCK), h * HEAD : (h + 1) * HEAD] = turn(t[:, h * HEAD : (h + 1) * HEAD], m)

        far_there(2, j)

        @pl.loop(0, BLOCKS)
        def _(m):
            @pl.when(j > 0)
            def _():
                part_copy(j, m, True).wait()

            t = _dot(a_s[at(m * BLOCK, BLOCK), at((1 - chip) * CHIP, CHIP)], wq_s[j, at((1 - chip) * CHIP, CHIP), :], 1, 0)
            queries(m, t + jnp.concatenate([mix_s[m, i, :HEAD, :] for i in range(HEADS)], 0))

        @pl.when(j == PIECES - 1)
        def _():
            residual.start()

        @pl.loop(0, BLOCKS)
        def _(qb):
            for k in range(BLOCKS):
                @pl.when(qb == k)
                def _():
                    events(j, ("diagonal", k), EVENTS)

            diagonal(g, qb)

        @pl.when(j >= 2)
        def _():
            away(j - 2).wait_send()

        last = FULL - 1 + chip * BLOCKS * BLOCKS
        for h in range(HEADS):
            score(g, 0, h)

        @pl.loop(0, STEPS)
        def _(t):
            for k in range(STEPS):
                todo = [(when, EVENTS[when, k]) for when in range(PIECES) if (when, k) in EVENTS]
                if todo:
                    @pl.when(t == k)
                    def _():
                        events(j, k, EVENTS)

            @pl.when((j < PIECES - 1) & (t == HAND))
            def _():
                for p in range(2):
                    hand_on(2, j + 1, p)

            ahead = t + 1 - FULL

            @pl.when((chip == 1) & (lax.rem(j, 2) == 0) & (ahead >= 0) & (ahead < BLOCKS * BLOCKS) & (lax.rem(ahead + BLOCKS * BLOCKS, BLOCKS) == 0))
            def _():
                for copy in kv_copies(g, lax.div(ahead, BLOCKS)):
                    copy.wait_recv()

            @pl.when(t <= last)
            def _():
                step(g, t, last)

        def finish(mine):
            core = c if mine else 1 - c

            @pl.loop(0, BLOCKS // 2)
            def _(i):
                qb = core * 2 + i
                for h in range(HEADS):
                    out = (mix_s[qb, h, :HEAD, :] * (1 / mix_s[qb, h, HEAD : HEAD + 1, :])).T.astype(jnp.bfloat16)
                    if mine:
                        o_s[at(i * BLOCK, BLOCK), at(c * 2048 + j * COLS + h * HEAD, HEAD)] = out
                    else:
                        pool_s[at(CHIP + lax.rem(j, 2) * OWN + i * BLOCK, BLOCK), h * HEAD : (h + 1) * HEAD] = out

        finish(False)
        away(j).start()
        finish(True)

        @pl.when(j < PIECES - 1)
        def _():
            for m in range(BLOCKS):
                part_copy(j + 1, m, True).start()

    for j in range(PIECES):
        sent(2, j)
    arrived(wo_far.at[at(sib * OWN, OWN), :], wown_send, wown_recv, to_sib)
    wo_load(0)
    residual.wait()
    for j in range(PIECES):
        arrived(o_s.at[:, at((1 - c) * 2048 + j * COLS, COLS)], o_send.at[j], o_recv.at[j], to_sib)

    def out_copy(n):
        return pltpu.make_async_copy(pool_s.at[at(lax.rem(n, 2) * OWN, OWN), pl.ds(0, WCOLS)], y_ref.at[:, cols_of(n)], out_sem.at[lax.rem(n, 2)])

    @pl.loop(0, WO)
    def _(n):
        for copy in wo_loads(n):
            copy.wait()

        @pl.when(n >= 2)
        def _():
            out_copy(n - 2).wait()

        slot = lax.rem(n, PIECES)

        @pl.loop(0, OWN // BLOCK)
        def _(m):
            @pl.when(m == 1)
            def _():
                @pl.when(n < WO - 1)
                def _():
                    wo_load(n + 1)

                events(n, "out", EVENTS)

            rows = at(m * BLOCK, BLOCK)
            t = a_s[rows, cols_of(n)].astype(jnp.float32) + _dot(o_s[rows, :], wq_s[slot, :, :WCOLS], 1, 0)
            pool_s[at(lax.rem(n, 2) * OWN + m * BLOCK, BLOCK), :WCOLS] = t.astype(jnp.bfloat16)

        out_copy(n).start()

    for n in range(WO - 2, WO):
        out_copy(n).wait()
    for j in range(2, PIECES):
        away(j).wait_send()

    @pl.when(chip == 0)
    def _():
        for g in range(2):
            for kb in range(BLOCKS):
                for copy in kv_copies(g, kb):
                    copy.wait_send()

    to_other.wait_send()
    wo_own.wait_send()
    for n in range(WO):
        wo_x(n).wait_send()
        wo_y(n).wait_send()
        for by_y in range(2):
            wo_c(n, by_y).wait_send()


HAND = 5
EVENTS = {
    (2, 15): [('x', 0)],
    (2, 20): [('x', 1)],
    (2, 21): [('y', 0)],
    (3, ('diagonal', 0)): [('y', 1), ('x', 2)],
    (3, ('diagonal', 3)): [('x', 3)],
    (3, 3): [('y', 2), ('x', 4)],
    (3, 7): [('y', 3), ('x', 5)],
    (3, 12): [('y', 4), ('x', 6)],
    (3, 16): [('y', 5), ('x', 7)],
    (3, 20): [('y', 6), ('x', 8)],
    (1, 'out'): [('y', 7), ('x', 9)],
    (3, 'out'): [('y', 8), ('x', 10)],
    (5, 'out'): [('y', 9), ('x', 11)],
    (7, 'out'): [('y', 10), ('x', 12)],
    (9, 'out'): [('y', 11), ('x', 13)],
    (10, 'out'): [('y', 12), ('x', 14)],
    (11, 'out'): [('y', 13), ('x', 15)],
    (12, 'out'): [('y', 14)],
    (13, 'out'): [('y', 15)],
}


def solution(mesh):
    dma = pltpu.SemaphoreType.DMA
    bf16, f32 = jnp.bfloat16, jnp.float32
    anywhere, vmem = pl.BlockSpec(memory_space=pl.ANY), pl.BlockSpec(memory_space=pltpu.VMEM)
    fused = pl.pallas_call(
        _kernel,
        in_specs=[anywhere, vmem, vmem, anywhere, anywhere, anywhere, anywhere],
        out_specs=[anywhere, anywhere, anywhere],
        out_shape=[jax.ShapeDtypeStruct((OWN, D), bf16), jax.ShapeDtypeStruct((D, D), bf16),
                   jax.ShapeDtypeStruct((PIECES - 1, BLOCKS, HEADS, HEAD, COLS), f32)],
        scratch_shapes=[
            pltpu.VMEM((CHIP, D), bf16),
            pltpu.VMEM((PIECES, D, COLS), bf16),
            pltpu.VMEM((D, COLS), bf16),
            pltpu.VMEM((2, 2 * CHIP, HEAD), bf16),
            pltpu.VMEM((2, HEAD + 16, 2 * CHIP), bf16),
            pltpu.VMEM((BLOCKS, HEADS, HEAD + 16, BLOCK), f32),
            pltpu.VMEM((BLOCKS, HEADS, BLOCK), f32),
            pltpu.VMEM((HEADS, BLOCK, BLOCK), f32),
            pltpu.VMEM((OWN, D), bf16),
            pltpu.VMEM((CHIP, HEAD), f32),
            pltpu.VMEM((CHIP, HEAD), f32),
            pltpu.VMEM((1, D), f32),
            dma((10, 2)), dma((10, 2)), dma((10, 2)), dma((10, 2)), dma((10,)), dma((10,)), dma((10,)), dma, dma, dma,
            dma((2, BLOCKS, 2)), dma((2, BLOCKS, 2)), dma((WO,)), dma((WO,)), dma((WO,)), dma((WO,)), dma((2, WO)), dma((2, WO)), dma, dma,
            dma((PIECES, 3)), dma((PIECES,)), dma((PIECES,)), dma, dma((2,)), dma((BLOCKS,)),
        ],
        compiler_params=pltpu.CompilerParams(collective_id=0, has_side_effects=True, vmem_limit_bytes=67043328),
        cost_estimate=pl.CostEstimate(flops=140 * 10**9, transcendentals=10**8, bytes_accessed=10**8),
    )

    freq = np.tile(float(THETA) ** (-np.arange(HEAD // 2) / (HEAD // 2)), 2)
    sign = np.where(np.arange(HEAD) < HEAD // 2, -1.0, 1.0)
    angles = [np.arange(64)[:, None] * n * freq for n in (64, 1)]
    turns = np.stack([f(t) for t in angles for f in (np.cos, lambda t: sign * np.sin(t))]).astype(np.float32)

    def step(x, gain, wq, wk, wv, wo):
        return fused(x, gain, turns, wq, wk, wv, wo)[0]

    tokens, whole = P(("dp", "sp"), None), P("sp", None)
    return jax.shard_map(
        step,
        mesh=mesh,
        in_specs=(tokens, P(None), whole, whole, whole, whole),
        out_specs=tokens,
        check_vma=False,
    )
```

```python
import jax
import jax.numpy as jnp
import numpy as np
from jax import lax
from jax.experimental import pallas as pl
from jax.experimental.pallas import tpu as pltpu
from jax.sharding import PartitionSpec as P

HEAD = 128
THETA = 10000
LOG2E = 1.4426950408889634
HIDDEN = -2e30
OWN = 1024
D = 4096
CHIP = 2 * OWN
HALF = OWN // 2
COLS = 512
PIECES = 4
BLOCK = 512
BLOCKS = CHIP // BLOCK
HEADS = COLS // HEAD
MESH = pl.DeviceIdType.MESH
E = HEAD**-0.5 * LOG2E
WCOLS = 256
WO = D // WCOLS
FULL = BLOCKS * (BLOCKS - 1) // 2
STEPS = FULL + BLOCKS * BLOCKS
PART = HALF // 2


def _dot(a, b, ca, cb):
    return lax.dot_general(a, b, (((ca,), (cb,)), ((), ())), preferred_element_type=jnp.float32)


def _kernel(x_ref, gain_ref, turns_ref, wq_ref, wk_ref, wv_ref, wo_ref, y_ref, wo_far, part_ref,
            a_s, wq_s, pool_s, k_s, v_s, mix_s, top_s, s_s, o_s, cos_s, sin_s, gain_s,
            x_send, x_recv, y_send, y_recv, c_send, c_recv, own_sem, tok_sem, tok_send, tok_recv,
            kv_send, kv_recv, wx_send, wx_recv, wy_send, wy_recv, wc_send, wc_recv, wown_send, wown_recv, w_sem,
            o_send, o_recv, res_sem, out_sem, part_sem):
    y, d = lax.axis_index("dp"), lax.axis_index("sp")
    c, chip = lax.rem(d, 2), lax.div(d, 2)
    sib = d + 1 - 2 * c
    far = 2 * (1 - chip)
    par = far + c
    to_y, to_sib = {"dp": 1 - y}, {"sp": sib}

    def at(i, n, unit=None):
        return pl.ds(pl.multiple_of(i, unit or n), n)

    def remote(src, dst, send, recv, device):
        return pltpu.make_async_remote_copy(src_ref=src, dst_ref=dst, send_sem=send, recv_sem=recv, device_id=device, device_id_type=MESH)

    def arrived(ref, send, recv, device):
        remote(ref, ref, send, recv, device).wait_recv()

    def source(item, j, core, rows):
        if item == 0:
            return wk_ref.at[rows, at(core * 256, 256)]
        if item == 1:
            return wv_ref.at[rows, at(core * 256, 256)]
        return wq_ref.at[rows, at(core * 2048 + j * COLS, COLS)]

    def place(item, j, rows):
        return wq_s.at[j, rows, :] if item == 2 else pool_s.at[rows, pl.ds(item * 256, 256)]

    def parts(item):
        return (0, 1) if item == 2 else (0,)

    def sem(item, j, p):
        return 2 + 2 * j + p if item == 2 else item

    def rows_of(item, device, half, p):
        n = PART if item == 2 else HALF
        return at(device * OWN + half * HALF + p * n, n)

    def x_copy(item, j, p, t):
        n = sem(item, j, p)
        return remote(source(item, j, t, rows_of(item, 0, y, p)), place(item, j, rows_of(item, d, y, p)), x_send.at[n, t], x_recv.at[n, c], {"sp": far + t})

    def send_x(item, j=0):
        for p in parts(item):
            for t in range(2):
                x_copy(item, j, p, t).start()

    def y_copy(item, j, p, s):
        n, here = sem(item, j, p), place(item, j, rows_of(item, far + s, y, p))
        return remote(here, here, y_send.at[n, s], y_recv.at[n, s], to_y)

    def hand_on(item, j, p):
        n = sem(item, j, p)
        for s in range(2):
            arrived(place(item, j, rows_of(item, far + s, y, p)), x_send.at[n, s], x_recv.at[n, s], {"sp": far + s})
            y_copy(item, j, p, s).start()

    def c_copy(item, j=0):
        n = sem(item, j, 0)
        return remote(source(item, j, 1 - c, pl.ds(0, OWN)), place(item, j, at(d * OWN, OWN)), c_send.at[n], c_recv.at[n], to_sib)

    def own_copy(item, j=0):
        return pltpu.make_async_copy(source(item, j, c, pl.ds(0, OWN)), place(item, j, at(d * OWN, OWN)), own_sem.at[sem(item, j, 0)])

    def near_there(item, j=0):
        n = sem(item, j, 0)
        own_copy(item, j).wait()
        arrived(place(item, j, at(sib * OWN, OWN)), c_send.at[n], c_recv.at[n], to_sib)

    def far_there(item, j=0):
        for p in parts(item):
            n = sem(item, j, p)
            for s in range(2):
                arrived(place(item, j, rows_of(item, far + s, 1 - y, p)), y_send.at[n, s], y_recv.at[n, s], to_y)

    def sent(item, j=0):
        c_copy(item, j).wait_send()
        for p in parts(item):
            for s in range(2):
                x_copy(item, j, p, s).wait_send()
                y_copy(item, j, p, s).wait_send()

    def cols_of(n):
        return at(n * WCOLS, WCOLS)

    def wo_x(n):
        return remote(wo_ref.at[at(y * HALF, HALF), cols_of(n)], wo_far.at[at(d * OWN + y * HALF, HALF), cols_of(n)], wx_send.at[n], wx_recv.at[n], {"sp": par})

    def wo_rows(owner, half, n):
        return wo_far.at[at(owner * OWN + half * HALF, HALF), cols_of(n)]

    def wo_y(n):
        return remote(wo_rows(par, y, n), wo_rows(par, y, n), wy_send.at[n], wy_recv.at[n], to_y)

    def wo_c(n, by_y):
        here = wo_rows(par, 1 - y if by_y else y, n)
        return remote(here, here, wc_send.at[by_y, n], wc_recv.at[by_y, n], to_sib)

    def wo_hand_x(n):
        arrived(wo_rows(par, y, n), wx_send.at[n], wx_recv.at[n], {"sp": par})
        wo_y(n).start()
        wo_c(n, 0).start()

    def wo_hand_y(n):
        arrived(wo_rows(par, 1 - y, n), wy_send.at[n], wy_recv.at[n], to_y)
        wo_c(n, 1).start()

    wo_own = remote(wo_ref, wo_far.at[at(d * OWN, OWN), :], wown_send, wown_recv, to_sib)

    def wo_loads(n):
        slot = lax.rem(n, PIECES)
        return [
            pltpu.make_async_copy(wo_ref.at[:, cols_of(n)], wq_s.at[slot, at(d * OWN, OWN), pl.ds(0, WCOLS)], w_sem.at[slot, 0]),
            pltpu.make_async_copy(wo_far.at[at(sib * OWN, OWN), cols_of(n)], wq_s.at[slot, at(sib * OWN, OWN), pl.ds(0, WCOLS)], w_sem.at[slot, 1]),
            pltpu.make_async_copy(wo_far.at[at(far * OWN, CHIP), cols_of(n)], wq_s.at[slot, at(far * OWN, CHIP), pl.ds(0, WCOLS)], w_sem.at[slot, 2]),
        ]

    def wo_load(n):
        for by_y in range(2):
            arrived(wo_rows(far + 1 - c, 1 - y if by_y else y, n), wc_send.at[by_y, n], wc_recv.at[by_y, n], to_sib)
        for copy in wo_loads(n):
            copy.start()

    barrier = pltpu.get_barrier_semaphore()
    for device in (to_sib, {"sp": far}, {"sp": far + 1}, to_y):
        pl.semaphore_signal(barrier, inc=1, device_id=device, device_id_type=MESH)
    tokens = pltpu.make_async_copy(x_ref, a_s.at[at(c * OWN, OWN), :], tok_sem)
    tokens.start()
    pl.semaphore_wait(barrier, 4)
    send_x(0)
    send_x(1)
    to_other = remote(x_ref, a_s.at[at(c * OWN, OWN), :], tok_send, tok_recv, to_sib)
    to_other.start()
    for item in range(2):
        c_copy(item).start()
        own_copy(item).start()
    for j in range(PIECES):
        c_copy(2, j).start()
        own_copy(2, j).start()
    wo_own.start()
    for g in range(2):
        v_s[g, HEAD:, :] = jnp.ones((16, 2 * CHIP), jnp.bfloat16)

    @pl.loop(0, CHIP // 64)
    def _(i):
        h = pl.ds(chip * (CHIP // 64) + i, 1)
        ch, sh, cl, sl = turns_ref[0, h, :], turns_ref[1, h, :], turns_ref[2], turns_ref[3]
        cos_s[at(i * 64, 64), :] = ch * cl - sh * sl
        sin_s[at(i * 64, 64), :] = sh * cl + ch * sl

    gain_s[...] = gain_ref[...].astype(jnp.float32).reshape(1, D)

    def norm(first):
        @pl.loop(0, OWN // 128)
        def _(i):
            rows = at(first + i * 128, 128)
            wide = a_s[rows, :].astype(jnp.float32)
            scale = lax.rsqrt(jnp.mean(wide * wide, -1, keepdims=True) + 1e-6)
            a_s[rows, :] = (wide * scale * gain_s[...]).astype(jnp.bfloat16)

    tokens.wait()
    norm(c * OWN)
    hand_on(0, 0, 0)
    send_x(2, 0)
    arrived(a_s.at[at((1 - c) * OWN, OWN), :], tok_send, tok_recv, to_sib)
    norm((1 - c) * OWN)
    hand_on(1, 0, 0)

    def turn(t, m):
        rows = at(m * BLOCK, BLOCK)
        return (t * cos_s[rows, :] + pltpu.roll(t, HEAD // 2, 1) * sin_s[rows, :]).astype(jnp.bfloat16)

    near_there(0)
    far_there(0)

    @pl.loop(0, BLOCKS)
    def _(m):
        t = _dot(a_s[at(m * BLOCK, BLOCK), :], pool_s[:, :256], 1, 0).astype(jnp.bfloat16).astype(jnp.float32)
        for g in range(2):
            k_s[g, at(chip * CHIP + m * BLOCK, BLOCK), :] = turn(t[:, g * HEAD : (g + 1) * HEAD], m)

    def part_copy(j, m, back):
        here, there = mix_s.at[m, :, pl.ds(0, HEAD), :], part_ref.at[j - 1, m]
        return pltpu.make_async_copy(there, here, part_sem.at[m]) if back else pltpu.make_async_copy(here, there, part_sem.at[m])

    def near_queries(j):
        near_there(2, j)

        @pl.loop(0, BLOCKS)
        def _(m):
            if j < PIECES - 1:
                part_copy(j + 1, m, False).wait()
            t = _dot(a_s[at(m * BLOCK, BLOCK), at(chip * CHIP, CHIP)], wq_s[j, at(chip * CHIP, CHIP), :], 1, 0)
            for i in range(HEADS):
                mix_s[m, i, :HEAD, :] = t[i * HEAD : (i + 1) * HEAD, :]
            if j:
                part_copy(j, m, False).start()

    send_x(2, 1)
    near_queries(3)
    hand_on(2, 0, 0)
    near_there(1)
    far_there(1)

    @pl.loop(0, BLOCKS)
    def _(m):
        t = _dot(a_s[at(m * BLOCK, BLOCK), :], pool_s[:, 256:], 1, 0)
        for g in range(2):
            v_s[g, :HEAD, at(chip * CHIP + m * BLOCK, BLOCK)] = t[:, g * HEAD : (g + 1) * HEAD].T.astype(jnp.bfloat16)

    def kv_copies(g, kb):
        keys = at(kb * BLOCK, BLOCK)
        return [
            remote(here, here, kv_send.at[g, kb, i], kv_recv.at[g, kb, i], {"sp": c + 2})
            for i, here in enumerate((k_s.at[g, keys, :], v_s.at[g, pl.ds(0, HEAD), keys]))
        ]

    def kv_go(g):
        @pl.when(chip == 0)
        def _():
            for kb in range(BLOCKS):
                for copy in kv_copies(g, kb):
                    copy.start()

    kv_go(0)
    send_x(2, 2)
    near_queries(2)
    hand_on(2, 0, 1)
    near_queries(1)
    near_queries(0)
    for item in range(2):
        sent(item)

    def diagonal(g, qb):
        half = BLOCK // 2
        at_keys = chip * CHIP + qb * BLOCK
        keys, values = k_s[g, at(at_keys, BLOCK), :], v_s[g, :, at(at_keys, BLOCK)]
        seen = lax.broadcasted_iota(jnp.int32, (half, half), 0) <= lax.broadcasted_iota(jnp.int32, (half, half), 1)
        for h in range(HEADS):
            q = pool_s[at(qb * BLOCK, BLOCK), h * HEAD : (h + 1) * HEAD]
            early, late = _dot(keys[:half], q, 1, 1), _dot(keys[half:], q[half:], 1, 1)
            left, late = jnp.where(seen, early[:, :half], HIDDEN), jnp.where(seen, late, HIDDEN)
            right = jnp.concatenate([early[:, half:], late], 0)
            for s, cols, n in ((left, pl.ds(0, half), half), (right, pl.ds(half, half), BLOCK)):
                top = s.max(axis=0, keepdims=True)
                top_s[qb, h : h + 1, cols] = top
                mix_s[qb, h, :, cols] = _dot(values[:, :n], jnp.exp2((s - top) * E).astype(jnp.bfloat16), 1, 0)

    def place_of(t):
        own_qb = 1 + jnp.where(t >= 1, 1, 0) + jnp.where(t >= 3, 1, 0)
        own_kb = t - jnp.where(t >= 1, 1, 0) - jnp.where(t >= 3, 2, 0) + chip * BLOCKS
        return jnp.where(t < FULL, own_qb, lax.rem(t + BLOCKS * BLOCKS - FULL, BLOCKS)), jnp.where(t < FULL, own_kb, lax.div(t - FULL, BLOCKS))

    def score(g, t, h):
        qb, kb = place_of(t)
        s_s[h] = _dot(k_s[g, at(kb * BLOCK, BLOCK), :], pool_s[at(qb * BLOCK, BLOCK), h * HEAD : (h + 1) * HEAD], 1, 1)

    def step(g, t, last):
        qb, kb = place_of(t)
        values = v_s[g, :, at(kb * BLOCK, BLOCK)]
        for h in range(HEADS):
            s = s_s[h]
            old = top_s[qb, h : h + 1, :]
            top = jnp.maximum(old, s.max(axis=0, keepdims=True))
            keep = jnp.exp2((old - top) * E)
            top_s[qb, h : h + 1, :] = top
            p = jnp.exp2((s - top) * E).astype(jnp.bfloat16)
            score(g, jnp.minimum(t + 1, last), h)
            mix_s[qb, h] = mix_s[qb, h] * keep + _dot(values, p, 1, 0)

    def away(j):
        here = pool_s.at[at(CHIP + lax.rem(j, 2) * OWN, OWN), :]
        return remote(here, o_s.at[:, at(c * 2048 + j * COLS, COLS)], o_send.at[j], o_recv.at[j], to_sib)

    residual = pltpu.make_async_copy(x_ref, a_s.at[pl.ds(0, OWN), :], res_sem)
    hand = {"x": wo_hand_x, "y": wo_hand_y}

    def send_wo(first, end):
        for n in range(first, end):
            wo_x(n).start()

    def events(j, point, table):
        for (when, place_), todo in table.items():
            if place_ == point:
                @pl.when((chip == 1) & (j == when))
                def _():
                    for kind, n in todo:
                        hand[kind](n)

    @pl.loop(0, PIECES)
    def _(j):
        g = lax.div(j, 2)
        @pl.when(j == 0)
        def _():
            kv_go(1)
            send_x(2, 3)

        @pl.when((chip == 1) & (j == 1))
        def _():
            send_wo(0, WO)

        @pl.when((chip == 0) & (j == 3))
        def _():
            send_wo(0, WO // 2)

        events(j, "start", EVENTS)

        def queries(m, t):
            t = t.astype(jnp.bfloat16).astype(jnp.float32)
            for h in range(HEADS):
                pool_s[at(m * BLOCK, BLOCK), h * HEAD : (h + 1) * HEAD] = turn(t[:, h * HEAD : (h + 1) * HEAD], m)

        far_there(2, j)

        @pl.loop(0, BLOCKS)
        def _(m):
            @pl.when(j > 0)
            def _():
                part_copy(j, m, True).wait()

            t = _dot(a_s[at(m * BLOCK, BLOCK), at((1 - chip) * CHIP, CHIP)], wq_s[j, at((1 - chip) * CHIP, CHIP), :], 1, 0)
            queries(m, t + jnp.concatenate([mix_s[m, i, :HEAD, :] for i in range(HEADS)], 0))

        @pl.when(j == PIECES - 1)
        def _():
            residual.start()

        @pl.loop(0, BLOCKS)
        def _(qb):
            for k in range(BLOCKS):
                @pl.when(qb == k)
                def _():
                    events(j, ("diagonal", k), EVENTS)

            diagonal(g, qb)

        @pl.when(j >= 2)
        def _():
            away(j - 2).wait_send()

        last = FULL - 1 + chip * BLOCKS * BLOCKS
        for h in range(HEADS):
            score(g, 0, h)

        @pl.loop(0, STEPS)
        def _(t):
            for k in range(STEPS):
                todo = [(when, EVENTS[when, k]) for when in range(PIECES) if (when, k) in EVENTS]
                if todo:
                    @pl.when(t == k)
                    def _():
                        events(j, k, EVENTS)

            @pl.when((j < PIECES - 1) & (t == HAND))
            def _():
                for p in range(2):
                    hand_on(2, j + 1, p)

            ahead = t + 1 - FULL

            @pl.when((chip == 1) & (lax.rem(j, 2) == 0) & (ahead >= 0) & (ahead < BLOCKS * BLOCKS) & (lax.rem(ahead + BLOCKS * BLOCKS, BLOCKS) == 0))
            def _():
                for copy in kv_copies(g, lax.div(ahead, BLOCKS)):
                    copy.wait_recv()

            @pl.when(t <= last)
            def _():
                step(g, t, last)

        def finish(mine):
            core = c if mine else 1 - c

            @pl.loop(0, BLOCKS // 2)
            def _(i):
                qb = core * 2 + i
                for h in range(HEADS):
                    out = (mix_s[qb, h, :HEAD, :] * (1 / mix_s[qb, h, HEAD : HEAD + 1, :])).T.astype(jnp.bfloat16)
                    if mine:
                        o_s[at(i * BLOCK, BLOCK), at(c * 2048 + j * COLS + h * HEAD, HEAD)] = out
                    else:
                        pool_s[at(CHIP + lax.rem(j, 2) * OWN + i * BLOCK, BLOCK), h * HEAD : (h + 1) * HEAD] = out

        finish(False)
        away(j).start()
        finish(True)

        @pl.when(j < PIECES - 1)
        def _():
            for m in range(BLOCKS):
                part_copy(j + 1, m, True).start()

    @pl.when(chip == 0)
    def _():
        send_wo(WO // 2, WO)
        for n in range(4):
            wo_hand_x(n)
        for n in range(2):
            wo_hand_y(n)

    for j in range(PIECES):
        sent(2, j)
    arrived(wo_far.at[at(sib * OWN, OWN), :], wown_send, wown_recv, to_sib)
    wo_load(0)
    residual.wait()
    for j in range(PIECES):
        arrived(o_s.at[:, at((1 - c) * 2048 + j * COLS, COLS)], o_send.at[j], o_recv.at[j], to_sib)

    def out_copy(n):
        return pltpu.make_async_copy(pool_s.at[at(lax.rem(n, 2) * OWN, OWN), pl.ds(0, WCOLS)], y_ref.at[:, cols_of(n)], out_sem.at[lax.rem(n, 2)])

    @pl.loop(0, WO)
    def _(n):
        for copy in wo_loads(n):
            copy.wait()

        @pl.when(n >= 2)
        def _():
            out_copy(n - 2).wait()

        slot = lax.rem(n, PIECES)

        @pl.loop(0, OWN // BLOCK)
        def _(m):
            @pl.when(m == 1)
            def _():
                @pl.when(n < WO - 1)
                def _():
                    wo_load(n + 1)

                events(n, "out", EVENTS)

                @pl.when((chip == 0) & (n < WO - 2))
                def _():
                    wo_hand_y(n + 2)

                @pl.when((chip == 0) & (n < WO - 4))
                def _():
                    wo_hand_x(n + 4)

            rows = at(m * BLOCK, BLOCK)
            t = a_s[rows, cols_of(n)].astype(jnp.float32) + _dot(o_s[rows, :], wq_s[slot, :, :WCOLS], 1, 0)
            pool_s[at(lax.rem(n, 2) * OWN + m * BLOCK, BLOCK), :WCOLS] = t.astype(jnp.bfloat16)

        out_copy(n).start()

    for n in range(WO - 2, WO):
        out_copy(n).wait()
    for j in range(2, PIECES):
        away(j).wait_send()

    @pl.when(chip == 0)
    def _():
        for g in range(2):
            for kb in range(BLOCKS):
                for copy in kv_copies(g, kb):
                    copy.wait_send()

    to_other.wait_send()
    wo_own.wait_send()
    for n in range(WO):
        wo_x(n).wait_send()
        wo_y(n).wait_send()
        for by_y in range(2):
            wo_c(n, by_y).wait_send()


HAND = 5
EVENTS = {
    (2, 15): [('x', 0)],
    (2, 20): [('x', 1)],
    (2, 21): [('y', 0)],
    (3, ('diagonal', 0)): [('y', 1), ('x', 2)],
    (3, ('diagonal', 3)): [('x', 3)],
    (3, 3): [('y', 2), ('x', 4)],
    (3, 7): [('y', 3), ('x', 5)],
    (3, 12): [('y', 4), ('x', 6)],
    (3, 16): [('y', 5), ('x', 7)],
    (3, 20): [('y', 6), ('x', 8)],
    (1, 'out'): [('y', 7), ('x', 9)],
    (3, 'out'): [('y', 8), ('x', 10)],
    (5, 'out'): [('y', 9), ('x', 11)],
    (7, 'out'): [('y', 10), ('x', 12)],
    (9, 'out'): [('y', 11), ('x', 13)],
    (10, 'out'): [('y', 12), ('x', 14)],
    (11, 'out'): [('y', 13), ('x', 15)],
    (12, 'out'): [('y', 14)],
    (13, 'out'): [('y', 15)],
}


def solution(mesh):
    dma = pltpu.SemaphoreType.DMA
    bf16, f32 = jnp.bfloat16, jnp.float32
    anywhere, vmem = pl.BlockSpec(memory_space=pl.ANY), pl.BlockSpec(memory_space=pltpu.VMEM)
    fused = pl.pallas_call(
        _kernel,
        in_specs=[anywhere, vmem, vmem, anywhere, anywhere, anywhere, anywhere],
        out_specs=[anywhere, anywhere, anywhere],
        out_shape=[jax.ShapeDtypeStruct((OWN, D), bf16), jax.ShapeDtypeStruct((D, D), bf16),
                   jax.ShapeDtypeStruct((PIECES - 1, BLOCKS, HEADS, HEAD, COLS), f32)],
        scratch_shapes=[
            pltpu.VMEM((CHIP, D), bf16),
            pltpu.VMEM((PIECES, D, COLS), bf16),
            pltpu.VMEM((D, COLS), bf16),
            pltpu.VMEM((2, 2 * CHIP, HEAD), bf16),
            pltpu.VMEM((2, HEAD + 16, 2 * CHIP), bf16),
            pltpu.VMEM((BLOCKS, HEADS, HEAD + 16, BLOCK), f32),
            pltpu.VMEM((BLOCKS, HEADS, BLOCK), f32),
            pltpu.VMEM((HEADS, BLOCK, BLOCK), f32),
            pltpu.VMEM((OWN, D), bf16),
            pltpu.VMEM((CHIP, HEAD), f32),
            pltpu.VMEM((CHIP, HEAD), f32),
            pltpu.VMEM((1, D), f32),
            dma((10, 2)), dma((10, 2)), dma((10, 2)), dma((10, 2)), dma((10,)), dma((10,)), dma((10,)), dma, dma, dma,
            dma((2, BLOCKS, 2)), dma((2, BLOCKS, 2)), dma((WO,)), dma((WO,)), dma((WO,)), dma((WO,)), dma((2, WO)), dma((2, WO)), dma, dma,
            dma((PIECES, 3)), dma((PIECES,)), dma((PIECES,)), dma, dma((2,)), dma((BLOCKS,)),
        ],
        compiler_params=pltpu.CompilerParams(collective_id=0, has_side_effects=True, vmem_limit_bytes=67043328),
        cost_estimate=pl.CostEstimate(flops=140 * 10**9, transcendentals=10**8, bytes_accessed=10**8),
    )

    freq = np.tile(float(THETA) ** (-np.arange(HEAD // 2) / (HEAD // 2)), 2)
    sign = np.where(np.arange(HEAD) < HEAD // 2, -1.0, 1.0)
    angles = [np.arange(64)[:, None] * n * freq for n in (64, 1)]
    turns = np.stack([f(t) for t in angles for f in (np.cos, lambda t: sign * np.sin(t))]).astype(np.float32)

    def step(x, gain, wq, wk, wv, wo):
        return fused(x, gain, turns, wq, wk, wv, wo)[0]

    tokens, whole = P(("dp", "sp"), None), P("sp", None)
    return jax.shard_map(
        step,
        mesh=mesh,
        in_specs=(tokens, P(None), whole, whole, whole, whole),
        out_specs=tokens,
        check_vma=False,
    )
```

```python
import jax
import jax.numpy as jnp
import numpy as np
from jax import lax
from jax.experimental import pallas as pl
from jax.experimental.pallas import tpu as pltpu
from jax.sharding import PartitionSpec as P

HEAD = 128
THETA = 10000
LOG2E = 1.4426950408889634
HIDDEN = -2e30
OWN = 1024
D = 4096
CHIP = 2 * OWN
HALF = OWN // 2
COLS = 512
PIECES = 4
BLOCK = 512
BLOCKS = CHIP // BLOCK
HEADS = COLS // HEAD
MESH = pl.DeviceIdType.MESH
E = HEAD**-0.5 * LOG2E
WCOLS = 256
WO = D // WCOLS
FULL = BLOCKS * (BLOCKS - 1) // 2
STEPS = FULL + BLOCKS * BLOCKS
PART = HALF // 2


def _dot(a, b, ca, cb):
    return lax.dot_general(a, b, (((ca,), (cb,)), ((), ())), preferred_element_type=jnp.float32)


def _kernel(x_ref, gain_ref, turns_ref, wq_ref, wk_ref, wv_ref, wo_ref, y_ref, wo_far, part_ref,
            a_s, wq_s, pool_s, k_s, v_s, mix_s, top_s, s_s, o_s, cos_s, sin_s, gain_s,
            x_send, x_recv, y_send, y_recv, c_send, c_recv, own_sem, tok_sem, tok_send, tok_recv,
            kv_send, kv_recv, wx_send, wx_recv, wy_send, wy_recv, wc_send, wc_recv, wown_send, wown_recv, w_sem,
            o_send, o_recv, res_sem, out_sem, part_sem):
    y, d = lax.axis_index("dp"), lax.axis_index("sp")
    c, chip = lax.rem(d, 2), lax.div(d, 2)
    sib = d + 1 - 2 * c
    far = 2 * (1 - chip)
    par = far + c
    to_y, to_sib = {"dp": 1 - y}, {"sp": sib}

    def at(i, n, unit=None):
        return pl.ds(pl.multiple_of(i, unit or n), n)

    def remote(src, dst, send, recv, device):
        return pltpu.make_async_remote_copy(src_ref=src, dst_ref=dst, send_sem=send, recv_sem=recv, device_id=device, device_id_type=MESH)

    def arrived(ref, send, recv, device):
        remote(ref, ref, send, recv, device).wait_recv()

    def source(item, j, core, rows):
        if item == 0:
            return wk_ref.at[rows, at(core * 256, 256)]
        if item == 1:
            return wv_ref.at[rows, at(core * 256, 256)]
        return wq_ref.at[rows, at(core * 2048 + j * COLS, COLS)]

    def place(item, j, rows):
        return wq_s.at[j, rows, :] if item == 2 else pool_s.at[rows, pl.ds(item * 256, 256)]

    def parts(item):
        return (0, 1) if item == 2 else (0,)

    def sem(item, j, p):
        return 2 + 2 * j + p if item == 2 else item

    def rows_of(item, device, half, p):
        n = PART if item == 2 else HALF
        return at(device * OWN + half * HALF + p * n, n)

    def x_copy(item, j, p, t):
        n = sem(item, j, p)
        return remote(source(item, j, t, rows_of(item, 0, y, p)), place(item, j, rows_of(item, d, y, p)), x_send.at[n, t], x_recv.at[n, c], {"sp": far + t})

    def send_x(item, j=0):
        for p in parts(item):
            for t in range(2):
                x_copy(item, j, p, t).start()

    def y_copy(item, j, p, s):
        n, here = sem(item, j, p), place(item, j, rows_of(item, far + s, y, p))
        return remote(here, here, y_send.at[n, s], y_recv.at[n, s], to_y)

    def hand_on(item, j, p):
        n = sem(item, j, p)
        for s in range(2):
            arrived(place(item, j, rows_of(item, far + s, y, p)), x_send.at[n, s], x_recv.at[n, s], {"sp": far + s})
            y_copy(item, j, p, s).start()

    def c_copy(item, j=0):
        n = sem(item, j, 0)
        return remote(source(item, j, 1 - c, pl.ds(0, OWN)), place(item, j, at(d * OWN, OWN)), c_send.at[n], c_recv.at[n], to_sib)

    def own_copy(item, j=0):
        return pltpu.make_async_copy(source(item, j, c, pl.ds(0, OWN)), place(item, j, at(d * OWN, OWN)), own_sem.at[sem(item, j, 0)])

    def near_there(item, j=0):
        n = sem(item, j, 0)
        own_copy(item, j).wait()
        arrived(place(item, j, at(sib * OWN, OWN)), c_send.at[n], c_recv.at[n], to_sib)

    def far_there(item, j=0):
        for p in parts(item):
            n = sem(item, j, p)
            for s in range(2):
                arrived(place(item, j, rows_of(item, far + s, 1 - y, p)), y_send.at[n, s], y_recv.at[n, s], to_y)

    def sent(item, j=0):
        c_copy(item, j).wait_send()
        for p in parts(item):
            for s in range(2):
                x_copy(item, j, p, s).wait_send()
                y_copy(item, j, p, s).wait_send()

    def cols_of(n):
        return at(n * WCOLS, WCOLS)

    def wo_x(n):
        return remote(wo_ref.at[at(y * HALF, HALF), cols_of(n)], wo_far.at[at(d * OWN + y * HALF, HALF), cols_of(n)], wx_send.at[n], wx_recv.at[n], {"sp": par})

    def wo_rows(owner, half, n):
        return wo_far.at[at(owner * OWN + half * HALF, HALF), cols_of(n)]

    def wo_y(n):
        return remote(wo_rows(par, y, n), wo_rows(par, y, n), wy_send.at[n], wy_recv.at[n], to_y)

    def wo_c(n, by_y):
        here = wo_rows(par, 1 - y if by_y else y, n)
        return remote(here, here, wc_send.at[by_y, n], wc_recv.at[by_y, n], to_sib)

    def wo_hand_x(n):
        arrived(wo_rows(par, y, n), wx_send.at[n], wx_recv.at[n], {"sp": par})
        wo_y(n).start()
        wo_c(n, 0).start()

    def wo_hand_y(n):
        arrived(wo_rows(par, 1 - y, n), wy_send.at[n], wy_recv.at[n], to_y)
        wo_c(n, 1).start()

    wo_own = remote(wo_ref, wo_far.at[at(d * OWN, OWN), :], wown_send, wown_recv, to_sib)

    def wo_loads(n):
        slot = lax.rem(n, PIECES)
        return [
            pltpu.make_async_copy(wo_ref.at[:, cols_of(n)], wq_s.at[slot, at(d * OWN, OWN), pl.ds(0, WCOLS)], w_sem.at[slot, 0]),
            pltpu.make_async_copy(wo_far.at[at(sib * OWN, OWN), cols_of(n)], wq_s.at[slot, at(sib * OWN, OWN), pl.ds(0, WCOLS)], w_sem.at[slot, 1]),
            pltpu.make_async_copy(wo_far.at[at(far * OWN, CHIP), cols_of(n)], wq_s.at[slot, at(far * OWN, CHIP), pl.ds(0, WCOLS)], w_sem.at[slot, 2]),
        ]

    def wo_load(n):
        for by_y in range(2):
            arrived(wo_rows(far + 1 - c, 1 - y if by_y else y, n), wc_send.at[by_y, n], wc_recv.at[by_y, n], to_sib)
        for copy in wo_loads(n):
            copy.start()

    barrier = pltpu.get_barrier_semaphore()
    for device in (to_sib, {"sp": far}, {"sp": far + 1}, to_y):
        pl.semaphore_signal(barrier, inc=1, device_id=device, device_id_type=MESH)
    tokens = pltpu.make_async_copy(x_ref, a_s.at[at(c * OWN, OWN), :], tok_sem)
    tokens.start()
    pl.semaphore_wait(barrier, 4)
    send_x(0)
    send_x(1)
    send_x(2, 0)
    send_x(2, 1)
    to_other = remote(x_ref, a_s.at[at(c * OWN, OWN), :], tok_send, tok_recv, to_sib)
    to_other.start()
    for item in range(2):
        c_copy(item).start()
        own_copy(item).start()
    for j in range(PIECES):
        c_copy(2, j).start()
        own_copy(2, j).start()
    wo_own.start()
    for g in range(2):
        v_s[g, HEAD:, :] = jnp.ones((16, 2 * CHIP), jnp.bfloat16)

    @pl.loop(0, CHIP // 64)
    def _(i):
        h = pl.ds(chip * (CHIP // 64) + i, 1)
        ch, sh, cl, sl = turns_ref[0, h, :], turns_ref[1, h, :], turns_ref[2], turns_ref[3]
        cos_s[at(i * 64, 64), :] = ch * cl - sh * sl
        sin_s[at(i * 64, 64), :] = sh * cl + ch * sl

    gain_s[...] = gain_ref[...].astype(jnp.float32).reshape(1, D)

    def norm(first):
        @pl.loop(0, OWN // 128)
        def _(i):
            rows = at(first + i * 128, 128)
            wide = a_s[rows, :].astype(jnp.float32)
            scale = lax.rsqrt(jnp.mean(wide * wide, -1, keepdims=True) + 1e-6)
            a_s[rows, :] = (wide * scale * gain_s[...]).astype(jnp.bfloat16)

    tokens.wait()
    norm(c * OWN)
    hand_on(0, 0, 0)
    arrived(a_s.at[at((1 - c) * OWN, OWN), :], tok_send, tok_recv, to_sib)
    norm((1 - c) * OWN)
    hand_on(1, 0, 0)

    def turn(t, m):
        rows = at(m * BLOCK, BLOCK)
        return (t * cos_s[rows, :] + pltpu.roll(t, HEAD // 2, 1) * sin_s[rows, :]).astype(jnp.bfloat16)

    near_there(0)
    far_there(0)

    @pl.loop(0, BLOCKS)
    def _(m):
        t = _dot(a_s[at(m * BLOCK, BLOCK), :], pool_s[:, :256], 1, 0).astype(jnp.bfloat16).astype(jnp.float32)
        for g in range(2):
            k_s[g, at(chip * CHIP + m * BLOCK, BLOCK), :] = turn(t[:, g * HEAD : (g + 1) * HEAD], m)

    def part_copy(j, m, back):
        here, there = mix_s.at[m, :, pl.ds(0, HEAD), :], part_ref.at[j - 1, m]
        return pltpu.make_async_copy(there, here, part_sem.at[m]) if back else pltpu.make_async_copy(here, there, part_sem.at[m])

    def near_queries(j):
        near_there(2, j)

        @pl.loop(0, BLOCKS)
        def _(m):
            if j < PIECES - 1:
                part_copy(j + 1, m, False).wait()
            t = _dot(a_s[at(m * BLOCK, BLOCK), at(chip * CHIP, CHIP)], wq_s[j, at(chip * CHIP, CHIP), :], 1, 0)
            for i in range(HEADS):
                mix_s[m, i, :HEAD, :] = t[i * HEAD : (i + 1) * HEAD, :]
            if j:
                part_copy(j, m, False).start()

    near_queries(3)
    hand_on(2, 0, 0)
    near_there(1)
    far_there(1)

    @pl.loop(0, BLOCKS)
    def _(m):
        t = _dot(a_s[at(m * BLOCK, BLOCK), :], pool_s[:, 256:], 1, 0)
        for g in range(2):
            v_s[g, :HEAD, at(chip * CHIP + m * BLOCK, BLOCK)] = t[:, g * HEAD : (g + 1) * HEAD].T.astype(jnp.bfloat16)

    def kv_copies(g, kb):
        keys = at(kb * BLOCK, BLOCK)
        return [
            remote(here, here, kv_send.at[g, kb, i], kv_recv.at[g, kb, i], {"sp": c + 2})
            for i, here in enumerate((k_s.at[g, keys, :], v_s.at[g, pl.ds(0, HEAD), keys]))
        ]

    def kv_go(g):
        @pl.when(chip == 0)
        def _():
            for kb in range(BLOCKS):
                for copy in kv_copies(g, kb):
                    copy.start()

    kv_go(0)
    send_x(2, 2)
    send_x(2, 3)
    kv_go(1)
    for n in range(WO):
        wo_x(n).start()
    near_queries(2)
    hand_on(2, 0, 1)
    near_queries(1)
    near_queries(0)
    for item in range(2):
        sent(item)

    def diagonal(g, qb):
        half = BLOCK // 2
        at_keys = chip * CHIP + qb * BLOCK
        keys, values = k_s[g, at(at_keys, BLOCK), :], v_s[g, :, at(at_keys, BLOCK)]
        seen = lax.broadcasted_iota(jnp.int32, (half, half), 0) <= lax.broadcasted_iota(jnp.int32, (half, half), 1)
        for h in range(HEADS):
            q = pool_s[at(qb * BLOCK, BLOCK), h * HEAD : (h + 1) * HEAD]
            early, late = _dot(keys[:half], q, 1, 1), _dot(keys[half:], q[half:], 1, 1)
            left, late = jnp.where(seen, early[:, :half], HIDDEN), jnp.where(seen, late, HIDDEN)
            right = jnp.concatenate([early[:, half:], late], 0)
            for s, cols, n in ((left, pl.ds(0, half), half), (right, pl.ds(half, half), BLOCK)):
                top = s.max(axis=0, keepdims=True)
                top_s[qb, h : h + 1, cols] = top
                mix_s[qb, h, :, cols] = _dot(values[:, :n], jnp.exp2((s - top) * E).astype(jnp.bfloat16), 1, 0)

    def place_of(t):
        own_qb = 1 + jnp.where(t >= 1, 1, 0) + jnp.where(t >= 3, 1, 0)
        own_kb = t - jnp.where(t >= 1, 1, 0) - jnp.where(t >= 3, 2, 0) + chip * BLOCKS
        return jnp.where(t < FULL, own_qb, lax.rem(t + BLOCKS * BLOCKS - FULL, BLOCKS)), jnp.where(t < FULL, own_kb, lax.div(t - FULL, BLOCKS))

    def score(g, t, h):
        qb, kb = place_of(t)
        s_s[h] = _dot(k_s[g, at(kb * BLOCK, BLOCK), :], pool_s[at(qb * BLOCK, BLOCK), h * HEAD : (h + 1) * HEAD], 1, 1)

    def step(g, t, last):
        qb, kb = place_of(t)
        values = v_s[g, :, at(kb * BLOCK, BLOCK)]
        for h in range(HEADS):
            s = s_s[h]
            old = top_s[qb, h : h + 1, :]
            top = jnp.maximum(old, s.max(axis=0, keepdims=True))
            keep = jnp.exp2((old - top) * E)
            top_s[qb, h : h + 1, :] = top
            p = jnp.exp2((s - top) * E).astype(jnp.bfloat16)
            score(g, jnp.minimum(t + 1, last), h)
            mix_s[qb, h] = mix_s[qb, h] * keep + _dot(values, p, 1, 0)

    def away(j):
        here = pool_s.at[at(CHIP + lax.rem(j, 2) * OWN, OWN), :]
        return remote(here, o_s.at[:, at(c * 2048 + j * COLS, COLS)], o_send.at[j], o_recv.at[j], to_sib)

    residual = pltpu.make_async_copy(x_ref, a_s.at[pl.ds(0, OWN), :], res_sem)
    hand = {"x": wo_hand_x, "y": wo_hand_y}

    def events(j, point, table):
        for (when, place_), todo in table.items():
            if place_ == point:
                @pl.when(j == when)
                def _():
                    for kind, n in todo:
                        hand[kind](n)

    @pl.loop(0, PIECES)
    def _(j):
        g = lax.div(j, 2)
        events(j, "start", EVENTS)

        def queries(m, t):
            t = t.astype(jnp.bfloat16).astype(jnp.float32)
            for h in range(HEADS):
                pool_s[at(m * BLOCK, BLOCK), h * HEAD : (h + 1) * HEAD] = turn(t[:, h * HEAD : (h + 1) * HEAD], m)

        far_there(2, j)

        @pl.loop(0, BLOCKS)
        def _(m):
            @pl.when(j > 0)
            def _():
                part_copy(j, m, True).wait()

            t = _dot(a_s[at(m * BLOCK, BLOCK), at((1 - chip) * CHIP, CHIP)], wq_s[j, at((1 - chip) * CHIP, CHIP), :], 1, 0)
            queries(m, t + jnp.concatenate([mix_s[m, i, :HEAD, :] for i in range(HEADS)], 0))

        @pl.when(j == PIECES - 1)
        def _():
            residual.start()

        @pl.loop(0, BLOCKS)
        def _(qb):
            for k in range(BLOCKS):
                @pl.when(qb == k)
                def _():
                    events(j, ("diagonal", k), EVENTS)

            diagonal(g, qb)

        @pl.when(j >= 2)
        def _():
            away(j - 2).wait_send()

        last = FULL - 1 + chip * BLOCKS * BLOCKS
        for h in range(HEADS):
            score(g, 0, h)

        @pl.loop(0, STEPS)
        def _(t):
            for k in range(STEPS):
                todo = [(when, EVENTS[when, k]) for when in range(PIECES) if (when, k) in EVENTS]
                if todo:
                    @pl.when(t == k)
                    def _():
                        events(j, k, EVENTS)

            @pl.when((j < PIECES - 1) & (t == HAND))
            def _():
                for p in range(2):
                    hand_on(2, j + 1, p)

            ahead = t + 1 - FULL

            @pl.when((chip == 1) & (lax.rem(j, 2) == 0) & (ahead >= 0) & (ahead < BLOCKS * BLOCKS) & (lax.rem(ahead + BLOCKS * BLOCKS, BLOCKS) == 0))
            def _():
                for copy in kv_copies(g, lax.div(ahead, BLOCKS)):
                    copy.wait_recv()

            @pl.when(t <= last)
            def _():
                step(g, t, last)

        def finish(mine):
            core = c if mine else 1 - c

            @pl.loop(0, BLOCKS // 2)
            def _(i):
                qb = core * 2 + i
                for h in range(HEADS):
                    out = (mix_s[qb, h, :HEAD, :] * (1 / mix_s[qb, h, HEAD : HEAD + 1, :])).T.astype(jnp.bfloat16)
                    if mine:
                        o_s[at(i * BLOCK, BLOCK), at(c * 2048 + j * COLS + h * HEAD, HEAD)] = out
                    else:
                        pool_s[at(CHIP + lax.rem(j, 2) * OWN + i * BLOCK, BLOCK), h * HEAD : (h + 1) * HEAD] = out

        finish(False)
        away(j).start()
        finish(True)

        @pl.when(j < PIECES - 1)
        def _():
            for m in range(BLOCKS):
                part_copy(j + 1, m, True).start()

    for j in range(PIECES):
        sent(2, j)
    arrived(wo_far.at[at(sib * OWN, OWN), :], wown_send, wown_recv, to_sib)
    wo_load(0)
    residual.wait()
    for j in range(PIECES):
        arrived(o_s.at[:, at((1 - c) * 2048 + j * COLS, COLS)], o_send.at[j], o_recv.at[j], to_sib)

    def out_copy(n):
        return pltpu.make_async_copy(pool_s.at[at(lax.rem(n, 2) * OWN, OWN), pl.ds(0, WCOLS)], y_ref.at[:, cols_of(n)], out_sem.at[lax.rem(n, 2)])

    @pl.loop(0, WO)
    def _(n):
        for copy in wo_loads(n):
            copy.wait()

        @pl.when(n >= 2)
        def _():
            out_copy(n - 2).wait()

        slot = lax.rem(n, PIECES)

        @pl.loop(0, OWN // BLOCK)
        def _(m):
            @pl.when(m == 1)
            def _():
                @pl.when(n < WO - 1)
                def _():
                    wo_load(n + 1)

                events(n, "out", EVENTS)

            rows = at(m * BLOCK, BLOCK)
            t = a_s[rows, cols_of(n)].astype(jnp.float32) + _dot(o_s[rows, :], wq_s[slot, :, :WCOLS], 1, 0)
            pool_s[at(lax.rem(n, 2) * OWN + m * BLOCK, BLOCK), :WCOLS] = t.astype(jnp.bfloat16)

        out_copy(n).start()

    for n in range(WO - 2, WO):
        out_copy(n).wait()
    for j in range(2, PIECES):
        away(j).wait_send()

    @pl.when(chip == 0)
    def _():
        for g in range(2):
            for kb in range(BLOCKS):
                for copy in kv_copies(g, kb):
                    copy.wait_send()

    to_other.wait_send()
    wo_own.wait_send()
    for n in range(WO):
        wo_x(n).wait_send()
        wo_y(n).wait_send()
        for by_y in range(2):
            wo_c(n, by_y).wait_send()


HAND = 1
EVENTS = {
    (2, 21): [('x', 0)],
    (3, ('diagonal', 0)): [('x', 1)],
    (3, ('diagonal', 2)): [('y', 0)],
    (3, 1): [('x', 2)],
    (3, 3): [('y', 1)],
    (3, 6): [('x', 3)],
    (3, 8): [('y', 2)],
    (3, 10): [('x', 4)],
    (3, 13): [('y', 3)],
    (3, 15): [('x', 5)],
    (3, 17): [('y', 4)],
    (3, 20): [('x', 6)],
    (0, 'out'): [('y', 5)],
    (1, 'out'): [('x', 7)],
    (2, 'out'): [('y', 6)],
    (3, 'out'): [('x', 8)],
    (5, 'out'): [('y', 7), ('x', 9)],
    (6, 'out'): [('y', 8), ('x', 10)],
    (7, 'out'): [('y', 9), ('x', 11)],
    (8, 'out'): [('y', 10), ('x', 12)],
    (9, 'out'): [('y', 11), ('x', 13)],
    (10, 'out'): [('y', 12), ('x', 14)],
    (11, 'out'): [('y', 13), ('x', 15)],
    (12, 'out'): [('y', 14)],
    (13, 'out'): [('y', 15)],
}


def solution(mesh):
    dma = pltpu.SemaphoreType.DMA
    bf16, f32 = jnp.bfloat16, jnp.float32
    anywhere, vmem = pl.BlockSpec(memory_space=pl.ANY), pl.BlockSpec(memory_space=pltpu.VMEM)
    fused = pl.pallas_call(
        _kernel,
        in_specs=[anywhere, vmem, vmem, anywhere, anywhere, anywhere, anywhere],
        out_specs=[anywhere, anywhere, anywhere],
        out_shape=[jax.ShapeDtypeStruct((OWN, D), bf16), jax.ShapeDtypeStruct((D, D), bf16),
                   jax.ShapeDtypeStruct((PIECES - 1, BLOCKS, HEADS, HEAD, COLS), f32)],
        scratch_shapes=[
            pltpu.VMEM((CHIP, D), bf16),
            pltpu.VMEM((PIECES, D, COLS), bf16),
            pltpu.VMEM((D, COLS), bf16),
            pltpu.VMEM((2, 2 * CHIP, HEAD), bf16),
            pltpu.VMEM((2, HEAD + 16, 2 * CHIP), bf16),
            pltpu.VMEM((BLOCKS, HEADS, HEAD + 16, BLOCK), f32),
            pltpu.VMEM((BLOCKS, HEADS, BLOCK), f32),
            pltpu.VMEM((HEADS, BLOCK, BLOCK), f32),
            pltpu.VMEM((OWN, D), bf16),
            pltpu.VMEM((CHIP, HEAD), f32),
            pltpu.VMEM((CHIP, HEAD), f32),
            pltpu.VMEM((1, D), f32),
            dma((10, 2)), dma((10, 2)), dma((10, 2)), dma((10, 2)), dma((10,)), dma((10,)), dma((10,)), dma, dma, dma,
            dma((2, BLOCKS, 2)), dma((2, BLOCKS, 2)), dma((WO,)), dma((WO,)), dma((WO,)), dma((WO,)), dma((2, WO)), dma((2, WO)), dma, dma,
            dma((PIECES, 3)), dma((PIECES,)), dma((PIECES,)), dma, dma((2,)), dma((BLOCKS,)),
        ],
        compiler_params=pltpu.CompilerParams(collective_id=0, has_side_effects=True, vmem_limit_bytes=67043328),
        cost_estimate=pl.CostEstimate(flops=140 * 10**9, transcendentals=10**8, bytes_accessed=10**8),
    )

    freq = np.tile(float(THETA) ** (-np.arange(HEAD // 2) / (HEAD // 2)), 2)
    sign = np.where(np.arange(HEAD) < HEAD // 2, -1.0, 1.0)
    angles = [np.arange(64)[:, None] * n * freq for n in (64, 1)]
    turns = np.stack([f(t) for t in angles for f in (np.cos, lambda t: sign * np.sin(t))]).astype(np.float32)

    def step(x, gain, wq, wk, wv, wo):
        return fused(x, gain, turns, wq, wk, wv, wo)[0]

    tokens, whole = P(("dp", "sp"), None), P("sp", None)
    return jax.shard_map(
        step,
        mesh=mesh,
        in_specs=(tokens, P(None), whole, whole, whole, whole),
        out_specs=tokens,
        check_vma=False,
    )
```
